32 devices in a mesh: rep: 2 (over x), dp: 16 (over y, z, core).
Axes of the slice: x: 2, y: 2, z: 4, core: 2. Of those that a mesh axis runs over, the one named last changes fastest.
Arguments:
- x: bfloat16 [32, 1024, 896], P(('rep', 'dp')), parts along dimension 0
- dy: bfloat16 [32, 1024, 896], P(('rep', 'dp')), parts along dimension 0
- w_gate: bfloat16 [2, 896, 4736], P(None, 'dp')
- w_up: bfloat16 [2, 896, 4736], P(None, 'dp')
- w_down: bfloat16 [2, 4736, 896], P(None, 'dp')
Outputs:
- output 1: bfloat16 [32, 1024, 896], P(('rep', 'dp')), parts along dimension 0
- output 2: bfloat16 [4, 896, 4736], P('rep', 'dp'), parts along dimension 0
- output 3: bfloat16 [4, 896, 4736], P('rep', 'dp'), parts along dimension 0
- output 4: bfloat16 [4, 4736, 896], P('rep', 'dp'), parts along dimension 0
There are 2 independent parts. The reference program is written for one: setup_inputs(seed, part) draws one part's arguments, and reference() takes and returns one part's arrays. A program takes and returns all parts, laid end to end along the dimension named above; an argument that names none is the same for every part.
All inputs are finite; a program needn't handle non-finite values.
Results may differ from the reference program's by a relative error of at most 0.018.
Values are sent between devices in bfloat16 or wider.
A program may use at most 2 GiB of HBM per device.

```python
import jax
import jax.numpy as jnp
from jax import lax

SEQUENCES = 16
TOKENS = 1024
D = 896
FF = 4736
LAYERS = 2
NAMES = ("w_gate", "w_up", "w_down")
SHAPES = {"w_gate": (LAYERS, D, FF), "w_up": (LAYERS, D, FF), "w_down": (LAYERS, FF, D)}


def bump(key, n, height):
    away = (jnp.arange(n, dtype=jnp.int32) - jax.random.randint(key, (), 0, n, jnp.int32)) % n
    return jnp.where(away < n // 8, height, 1.0)


def together(key, own, strength):
    shared = jax.random.normal(key, own.shape[1:], jnp.float32)
    return (own + strength * shared) * lax.rsqrt(1 + strength * strength)


def setup_inputs(seed: int = 0, part: int = 0) -> dict:
    kx, kdy, ka, kb, kz, kf, kh, kl, *kw = jax.random.split(jax.random.key(seed), 8 + len(NAMES))
    kx, kdy, ka, kb = (jax.random.fold_in(k, part) for k in (kx, kdy, ka, kb))
    shape = (SEQUENCES, TOKENS, D)
    much_x, much_dy = jax.random.uniform(kz, (2,), jnp.float32, 0.0, 1.0)
    layers = 2.0 ** jax.random.uniform(kl, (LAYERS, 1, 1), jnp.float32, -1.0, 1.0)
    x = together(ka, jax.random.normal(kx, shape, jnp.float32), much_x) * bump(kf, D, 4.0)
    dy = together(kb, jax.random.normal(kdy, shape, jnp.float32), much_dy)
    drawn = {"x": x.astype(jnp.bfloat16), "dy": (dy * (SEQUENCES * TOKENS) ** -0.5).astype(jnp.bfloat16)}
    for key, name in zip(kw, NAMES, strict=True):
        w = jax.random.normal(key, SHAPES[name], jnp.float32) * SHAPES[name][1] ** -0.5
        drawn[name] = (w * {"w_gate": 1.0, "w_up": bump(kh, FF, 4.0), "w_down": layers}[name]).astype(jnp.bfloat16)
    return drawn


def matmul(a, w):
    return jnp.dot(a, w, preferred_element_type=jnp.float32).astype(jnp.bfloat16)


def normed(h):
    wide = h.astype(jnp.float32)
    scale = lax.rsqrt(jnp.mean(wide**2, -1, keepdims=True) + 1e-6)
    return (wide * scale).astype(jnp.bfloat16)


def layer(h, w):
    a = normed(h)
    gate = jnp.dot(a, w["w_gate"], preferred_element_type=jnp.float32)
    up = jnp.dot(a, w["w_up"], preferred_element_type=jnp.float32)
    return h + matmul((jax.nn.silu(gate) * up).astype(jnp.bfloat16), w["w_down"])


def stack(weights, h):
    return lax.scan(lambda h, w: (layer(h, w), None), h, weights)[0]


def reference(x, dy, w_gate, w_up, w_down):
    weights = dict(zip(NAMES, (w_gate, w_up, w_down), strict=True))

    def take(so_far, sequence):
        h, by_y = sequence
        _, back = jax.vjp(stack, weights, h)
        by_weights, by_h = back(by_y)
        return jax.tree.map(lambda total, term: total + term.astype(jnp.float32), so_far, by_weights), by_h

    none_yet = {name: jnp.zeros(w.shape, jnp.float32) for name, w in weights.items()}
    by_weights, by_x = lax.scan(take, none_yet, (x, dy))
    return (by_x, *(by_weights[name].astype(jnp.bfloat16) for name in NAMES))
```

```python
import functools

import jax
import jax.numpy as jnp
from jax import lax
from jax.experimental import pallas as pl
from jax.experimental.pallas import tpu as pltpu
from jax.sharding import PartitionSpec as P

MESH = pl.DeviceIdType.MESH
BF16, F32 = jnp.bfloat16, jnp.float32
LAYERS, T, D, FF = 2, 1024, 896, 4736
N = 16
TILE = 256
TILES = 19
FFP = TILE * TILES
RG, RD = D // N, FF // N
EPS = 1e-6
CH = 128
ROW_CHUNKS = 2
ROWS = T // ROW_CHUNKS

GU_B, GU_A = 1664, 1536
D_B, D_A = 104, 96
D_SUBS_B, D_SUBS_A = ((0, 56), (56, 48)), ((0, 48), (48, 48))


class Place:
    def __init__(self):
        self.rep = lax.axis_index("rep")
        me = lax.axis_index("dp")
        self.core = lax.rem(me, 2)
        self.chip = me // 2
        self.ring = jnp.where(self.chip < 4, self.chip, 11 - self.chip)
        self.way = 1 - 2 * self.core
        self.next = (self.rep, self.device(1))
        self.prev = (self.rep, self.device(-1))
        self.sibling = (self.rep, self.chip * 2 + 1 - self.core)
        self.other = (1 - self.rep, me)

    def chip_at(self, steps):
        r = lax.rem(self.ring + self.way * steps + 16, 8)
        return jnp.where(r < 4, r, 11 - r)

    def device(self, steps):
        return self.chip_at(steps) * 2 + self.core


def barrier(devices):
    sem = pltpu.get_barrier_semaphore()
    for device in devices:
        pl.semaphore_signal(sem, inc=1, device_id=device, device_id_type=MESH)
    pl.semaphore_wait(sem, len(devices))


def remote(src, dst, send, recv, device):
    return pltpu.make_async_remote_copy(
        src_ref=src, dst_ref=dst, send_sem=send, recv_sem=recv, device_id=device, device_id_type=MESH
    )


def loop(lo, hi, body):
    def run(i, carry):
        body(i)
        return carry

    lax.fori_loop(lo, hi, run, 0)


def start(copies):
    for copy in copies:
        copy.start()


def wait(copies):
    for copy in copies:
        copy.wait()


def mult(x, m):
    return pl.multiple_of(x, m)


def dot(a, b, dims=((1,), (0,))):
    return lax.dot_general(a, b, (dims, ((), ())), preferred_element_type=F32)


def forward_kernel(
    x_ref, wg_ref, wu_ref, wd_ref,
    g_out, d_out, p_out, q_out, actt_out, at_out, h1_out,
    a_s, h_s, hacc, wgu_t, wd_t, p_s, q_s, pt_s, at_s, zc, zr,
    ring_recv, x_recv, sib_recv, ring_send, x_send, sib_send, local_sem, w_sem, o_sem, at_sem,
):
    here = Place()
    barrier((here.next, here.prev, here.sibling, here.other))

    def gu_part(ref, dev, a_group):
        rows = pl.ds(mult(dev * RG, 8), RG)
        if a_group is None:
            return ref.at[rows, pl.ds(0, GU_B)]
        return ref.at[rows, pl.ds(mult(GU_B + GU_A * a_group, 128), GU_A)]

    def d_part(ref, dev, a_group, sub):
        if a_group is None:
            start, size = D_SUBS_B[sub]
        else:
            start, size = D_SUBS_A[sub]
            start = D_B + D_A * a_group + start
        return ref.at[pl.ds(mult(dev * RD + start, 8), size), :]

    GU_ITEMS = ((0, False, 0, 0), (1, False, 0, 0), (0, True, 0, 1), (1, True, 0, 1))
    D_ITEMS = ((2, False, 0, 0), (2, True, 0, 2), (2, False, 1, 1), (2, True, 1, 3))

    def region(l, item, dev, group):
        mat, own, sub, _ = item
        if mat < 2:
            return gu_part(g_out.at[l, mat], dev, group if own else None)
        return d_part(d_out.at[l], dev, group if own else None, sub)

    def rr(l, mat, t, slot):
        return ring_recv.at[((l * 3 + mat) * 7 + t - 1) * 4 + slot]

    def xr(l, mat, t, sub):
        return x_recv.at[((l * 3 + mat) * 7 + t - 1) * 2 + sub]

    def lm(l, mat):
        return l * 3 + mat

    def to_sibling(l, mat, src, dst):
        remote(src, dst, sib_send.at[lm(l, mat)], sib_recv.at[lm(l, mat)], here.sibling).start()

    def ring_event(l, t, item):
        mat, own, sub, slot = item
        reg = region(l, item, here.device(-t), here.rep)
        remote(reg, reg, ring_send.at[lm(l, mat)], rr(l, mat, t, slot), here.next).wait_recv()

        @pl.when(t < 7)
        def _():
            remote(reg, reg, ring_send.at[lm(l, mat)], rr(l, mat, t + 1, slot), here.next).start()

        if own:
            remote(reg, reg, x_send.at[lm(l, mat)], xr(l, mat, t, sub), here.other).start()
        to_sibling(l, mat, reg, reg)

    def x_event(l, t, item):
        mat, _, sub, _ = item
        reg = region(l, item, here.device(-t), 1 - here.rep)
        remote(reg, reg, x_send.at[lm(l, mat)], xr(l, mat, t, sub), here.other).wait_recv()
        to_sibling(l, mat, reg, reg)

    def x_events(l, t, items):
        for item in items:
            if item[1]:
                x_event(l, t, item)

    def start_own(l, mats):
        me = here.device(0)
        for mat in mats:
            src = (wg_ref, wu_ref, wd_ref)[mat].at[l]
            items = [i for i in GU_ITEMS + D_ITEMS if i[0] == mat]
            for item in items:
                _, own, sub, slot = item
                group = here.rep if own else None
                part = gu_part(src, 0, group) if mat < 2 else d_part(src, 0, group, sub)
                remote(
                    part, region(l, item, me, here.rep), ring_send.at[lm(l, mat)], rr(l, mat, 1, slot), here.next
                ).start()
        for mat in mats:
            src = (wg_ref, wu_ref, wd_ref)[mat].at[l]
            if mat < 2:
                whole = g_out.at[l, mat, pl.ds(mult(me * RG, 8), RG), pl.ds(0, FF)]
            else:
                whole = d_out.at[l, pl.ds(mult(me * RD, 8), RD), :]
            to_sibling(l, mat, src, whole)
            pltpu.make_async_copy(src, whole, local_sem.at[lm(l, mat)]).start()

    def wait_own(l, mats):
        for mat in mats:
            src = (wg_ref, wu_ref, wd_ref)[mat].at[l]
            pltpu.make_async_copy(src, src, local_sem.at[lm(l, mat)]).wait()

    def wait_sibling(l, mat):
        half = g_out.at[l, mat, pl.ds(0, D // 2), pl.ds(0, FF)] if mat < 2 else d_out.at[l, pl.ds(0, FF // 2), :]
        remote(half, half, sib_send.at[lm(l, mat)], sib_recv.at[lm(l, mat)], here.sibling).wait_recv()

    def wait_sends(l):
        for mat in range(3):
            if mat < 2:
                rows = pl.ds(0, 7 * RG)
                sent = [g_out.at[l, mat, rows, pl.ds(0, GU_B + GU_A)], g_out.at[l, mat, rows, pl.ds(0, GU_A)]]
                half = g_out.at[l, mat, pl.ds(0, D // 2), pl.ds(0, FF)]
            else:
                sent = [d_out.at[l, pl.ds(0, 7 * (D_B + D_A)), :], d_out.at[l, pl.ds(0, 7 * D_A), :]]
                half = d_out.at[l, pl.ds(0, FF // 2), :]
            for ref, sem in zip(sent + [half], (ring_send, x_send, sib_send)):
                remote(ref, ref, sem.at[lm(l, mat)], sem.at[lm(l, mat)], here.next).wait_send()

    start_own(0, (0, 1, 2))

    zc[...] = jnp.zeros_like(zc)
    zr[...] = jnp.zeros_like(zr)
    pads = [(zc, g_out.at[l, m, :, pl.ds(FF, FFP - FF)]) for l in range(LAYERS) for m in range(2)]
    pads += [(zr, d_out.at[l, pl.ds(FF, FFP - FF), :]) for l in range(LAYERS)]
    for i, (src, dst) in enumerate(pads):
        pltpu.make_async_copy(src, dst, local_sem.at[6 + i]).start()

    def norm(src):
        def chunk(i):
            rows = pl.ds(mult(i * CH, CH), CH)
            wide = src[rows, :].astype(F32)
            a = wide * lax.rsqrt(jnp.mean(wide * wide, -1, keepdims=True) + EPS)
            a_s[rows, :] = a.astype(BF16)
            at_s[:, rows] = a.astype(BF16).T

        loop(0, T // CH, chunk)

    def put_at(l):
        return pltpu.make_async_copy(at_s, at_out.at[l], at_sem)

    norm(x_ref)
    put_at(0).start()

    def first(t):
        for item in GU_ITEMS + D_ITEMS:
            ring_event(0, t, item)

        @pl.when(t == 6)
        def _():
            start_own(1, (0, 1))

        @pl.when(t > 1)
        def _():
            x_events(0, t - 1, GU_ITEMS + D_ITEMS)

    loop(1, 8, first)
    x_events(0, 7, GU_ITEMS + D_ITEMS)
    for i, (src, dst) in enumerate(pads):
        pltpu.make_async_copy(src, dst, local_sem.at[6 + i]).wait()
    wait_own(0, (0, 1, 2))
    for mat in range(3):
        wait_sibling(0, mat)

    def layer(l, items, after_six):
        with_h = l == 0

        def loads(j, slot):
            cols = pl.ds(mult(j * TILE, TILE), TILE)
            pairs = [(g_out.at[l, m, :, cols], wgu_t.at[slot, :, pl.ds(m * TILE, TILE)]) for m in range(2)]
            if with_h:
                pairs.append((d_out.at[l, cols, :], wd_t.at[slot]))
            return [pltpu.make_async_copy(src, dst, w_sem.at[slot, i]) for i, (src, dst) in enumerate(pairs)]

        def stores(j, slot):
            rows = pl.ds(mult(j * TILE, TILE), TILE)
            pairs = ((p_s, p_out.at[l, j]), (q_s, q_out.at[l, j]), (pt_s, actt_out.at[l, rows, :]))
            return [pltpu.make_async_copy(src.at[slot], dst, o_sem.at[slot, i]) for i, (src, dst) in enumerate(pairs)]

        start(loads(0, 0))

        def tick(j):
            slot = lax.rem(j, 2)

            @pl.when(j + 1 < TILES)
            def _():
                start(loads(j + 1, 1 - slot))

            wait(loads(j, slot))

            @pl.when(j >= 2)
            def _():
                wait(stores(j - 2, slot))

            for r in range(ROW_CHUNKS):
                rows = pl.ds(r * ROWS, ROWS)
                both = dot(a_s[rows, :], wgu_t[slot])
                gate, up = both[:, :TILE], both[:, TILE:]
                s = 0.5 * jnp.tanh(0.5 * gate) + 0.5
                q = gate * s
                q_s[slot, rows, :] = q
                p_s[slot, rows, :] = up * (s + q * (1 - s))
                prod = (q * up).astype(BF16)
                pt_s[slot, :, rows] = prod.T
                if with_h:
                    hacc[rows, :] += dot(prod, wd_t[slot])
            start(stores(j, slot))

            def event(e):
                t = e // 4 + 1
                for i, item in enumerate(items):
                    pl.when(lax.rem(e, 4) == i)(functools.partial(ring_event, 1, t, item))
                pl.when(e == 4 * 6 - 1)(after_six)
                pl.when((lax.rem(e, 4) == 3) & (t > 1))(functools.partial(x_events, 1, t - 1, items))

            loop((j * 28) // TILES, ((j + 1) * 28) // TILES, event)

        loop(0, TILES, tick)
        x_events(1, 7, items)
        for j in (TILES - 2, TILES - 1):
            wait(stores(j, j % 2))

    hacc[...] = jnp.zeros_like(hacc)
    layer(0, GU_ITEMS, lambda: start_own(1, (2,)))

    def new_h(i):
        rows = pl.ds(mult(i * CH, CH), CH)
        y = hacc[rows, :].astype(BF16)
        h_s[rows, :] = (x_ref[rows, :].astype(F32) + y.astype(F32)).astype(BF16)

    loop(0, T // CH, new_h)
    put_h = pltpu.make_async_copy(h_s, h1_out, at_sem)
    put_at(0).wait()
    norm(h_s)
    put_h.start()
    put_h.wait()
    put_at(1).start()
    wait_own(1, (0, 1))
    wait_sibling(1, 0)
    wait_sibling(1, 1)
    layer(1, D_ITEMS, lambda: None)
    wait_own(1, (2,))
    wait_sibling(1, 2)
    put_at(1).wait()
    for l in range(LAYERS):
        wait_sends(l)


def forward(x, wg, wu, wd):
    any_, vmem = pl.BlockSpec(memory_space=pl.ANY), pl.BlockSpec(memory_space=pltpu.VMEM)
    dma = pltpu.SemaphoreType.DMA
    return pl.pallas_call(
        forward_kernel,
        out_shape=(
            jax.ShapeDtypeStruct((LAYERS, 2, D, FFP), BF16),
            jax.ShapeDtypeStruct((LAYERS, FFP, D), BF16),
            jax.ShapeDtypeStruct((LAYERS, TILES, T, TILE), F32),
            jax.ShapeDtypeStruct((LAYERS, TILES, T, TILE), F32),
            jax.ShapeDtypeStruct((LAYERS, FFP, T), BF16),
            jax.ShapeDtypeStruct((LAYERS, D, T), BF16),
            jax.ShapeDtypeStruct((T, D), BF16),
        ),
        in_specs=[vmem] * 4,
        out_specs=(any_,) * 7,
        scratch_shapes=[
            pltpu.VMEM((T, D), BF16),
            pltpu.VMEM((T, D), BF16),
            pltpu.VMEM((T, D), F32),
            pltpu.VMEM((2, D, 2 * TILE), BF16),
            pltpu.VMEM((2, TILE, D), BF16),
            pltpu.VMEM((2, T, TILE), F32),
            pltpu.VMEM((2, T, TILE), F32),
            pltpu.VMEM((2, TILE, T), BF16),
            pltpu.VMEM((D, T), BF16),
            pltpu.VMEM((D, FFP - FF), BF16),
            pltpu.VMEM((FFP - FF, D), BF16),
            dma((2 * 3 * 7 * 4,)),
            dma((2 * 3 * 7 * 2,)),
            dma((6,)),
            dma((6,)),
            dma((6,)),
            dma((6,)),
            dma((12,)),
            dma((2, 3)),
            dma((2, 3)),
            dma(()),
        ],
        compiler_params=pltpu.CompilerParams(
            collective_id=0, has_side_effects=True, vmem_limit_bytes=56 * 1024 * 1024
        ),
        name="forward_gather",
    )(x, wg, wu, wd)


PAIRS, STEPS, PLACES = 6, 8, 4
PER_PAIR = STEPS // 2 * PLACES
D_PART, C_PART = 72, 5 * TILE
D_LAST, C_LAST = RD - 3 * D_PART, FF - 3 * C_PART
D_PAIRS = 2
LAST_EVENT = (LAYERS * PAIRS + 1) * PER_PAIR
AHEAD = PLACES - 1
LAG = 2 * PLACES
FIRST_EVENT = 2
PAIR_EVENTS, TILE_EVENTS = 12, 54


def backward_kernel(
    dy_ref, x_ref, h1_ref, g_ref, d_ref, p_ref, q_ref, actt_ref, at_ref,
    dx_out, dgu_out, dd_out, own_gu, sib_gu, own_d, sib_d,
    dh_s, at_s, h_s, dacc, lhs_t, blk_s, wgu_t, wd_t, p_t, q_t, dz_s, term_s, slot_d, slot_c, st_d, st_c,
    ring_recv, ring_send, st_sem, fin_sem, sd_recv, sgu_recv, lhs_sem, blk_sem, blk_send, w_sem, term_sem, term_send, misc_sem,
):
    here = Place()
    barrier((here.next, here.prev, here.sibling))

    def chips(s):
        return here.chip_at(-1 - s), here.chip_at(1 + s)

    class Lane:
        def __init__(self, l, pair, lane, s, place, down, last):
            chip, _ = chips(s)
            self.s, self.place = s, place
            self.sems = [sem.at[l, pair, lane] for sem in (ring_recv, ring_send)]
            self.fin = fin_sem.at[l, pair, lane]
            if down:
                part = pair * 2 + lane
                rows, cut = (pl.ds(first, D_LAST if last else D_PART) for first in (mult(part * D_PART, 8), 0))
                self.slots = [slot_d.at[pair, lane, to, cut, :] for to in (s, s + 1)]
                self.st = [st_d.at[place, i, cut, :] for i in range(2)]
                self.terms = [ref.at[l, chip, rows, :] for ref in (own_d, sib_d)]
                self.result = dd_out.at[l, rows, :]
            else:
                part = pair - D_PAIRS
                cols, cut = (pl.ds(first, C_LAST if last else C_PART) for first in (mult(part * C_PART, 128), 0))
                self.slots = [slot_c.at[part, lane, to, :, cut] for to in (s, s + 1)]
                self.st = [st_c.at[place, i, :, cut] for i in range(2)]
                self.terms = [ref.at[l, lane, chip, :, cols] for ref in (own_gu, sib_gu)]
                self.result = dgu_out.at[lane, l, :, cols]

        def stage(self):
            pairs = zip(self.terms, self.st)
            return [pltpu.make_async_copy(a, b, st_sem.at[self.place, i]) for i, (a, b) in enumerate(pairs)]

        def send(self, to):
            recv, sent = self.sems
            return remote(self.slots[0], self.slots[to], sent.at[self.s], recv.at[self.s + to], here.next)

        def finish(self):
            return pltpu.make_async_copy(self.slots[0], self.result, self.fin)

        def step(self):
            wait(self.stage())
            slot = self.slots[0]
            ends = [st[...].astype(F32) for st in self.st]

            @pl.when(self.s > 0)
            def _():
                self.send(0).wait_recv()
                slot[...] = (slot[...].astype(F32) + (ends[0] + ends[1])).astype(BF16)

            @pl.when(self.s == 0)
            def _():
                slot[...] = (ends[0] + ends[1]).astype(BF16)

            pl.when(self.s < STEPS - 1)(lambda: self.send(1).start())
            pl.when(self.s == STEPS - 1)(lambda: self.finish().start())

        def wait_out(self):
            pl.when(self.s < STEPS - 1)(lambda: self.send(1).wait_send())
            pl.when(self.s == STEPS - 1)(lambda: self.finish().wait())

        def prefetch(self):
            start(self.stage())

    def with_lane(e, action, ahead_of=lambda l, pair, lane, s: None):
        round_, place = e // PLACES, lax.rem(e, PLACES)
        new = place // 2
        index = round_ // PLACES + new - 1
        s = lax.rem(round_, PLACES) + PLACES * (1 - new)
        lane = lax.rem(place, 2)

        @pl.when((index >= 0) & (index < LAYERS * PAIRS))
        def _():
            behind = jnp.where(index < PAIRS, 0, 1)
            l, pair = 1 - behind, index - PAIRS * behind
            ahead_of(l, pair, lane, s)
            down = pair < D_PAIRS
            last_d = (pair == D_PAIRS - 1) & (lane == 1)
            last_c = pair == PAIRS - 1
            for is_down, is_last, chosen in (
                (True, False, down & ~last_d), (True, True, last_d),
                (False, False, ~down & ~last_c), (False, True, last_c),
            ):
                pl.when(chosen)(lambda: action(Lane(l, pair, lane, s, place, is_down, is_last)))

    def terms_ready(l, pair, lane, s):
        @pl.when((pair == 0) & (lane == 0))
        def _():
            whole = sib_d.at[l, 0]
            remote(whole, whole, blk_send.at[0], sd_recv.at[l, s], here.sibling).wait_recv()

        @pl.when((pair >= D_PAIRS) & (lane == 0) & (s == 0))
        def _():
            for is_last in (False, True):
                width = FFP - 3 * C_PART if is_last else C_PART

                @pl.when((pair == PAIRS - 1) == is_last)
                def _(width=width):
                    part = sib_gu.at[l, :, :, :, pl.ds(0, width)]
                    sem = sgu_recv.at[l, pair - D_PAIRS]
                    remote(part, part, term_send.at[0, 0], sem, here.sibling).wait_recv()

    def fetch(e):
        with_lane(e, Lane.prefetch, terms_ready)

    def event(e):
        pl.when(e >= LAG)(lambda: with_lane(e - LAG, Lane.wait_out))
        fetch(e + AHEAD)
        with_lane(e, Lane.step)

    def lhs_loads(l, s, slot):
        mine, other = chips(s)
        rows = ((mine * 2 + here.core) * RD, (other * 2 + 1 - here.core) * RD)
        return [
            pltpu.make_async_copy(actt_ref.at[l, pl.ds(mult(row, 8), RD), :], lhs_t.at[slot, i], lhs_sem.at[slot, i])
            for i, row in enumerate(rows)
        ]

    def block_copies(l, s, slot):
        mine, other = chips(s)
        return (
            pltpu.make_async_copy(blk_s.at[slot, 0], own_d.at[l, mine], blk_sem.at[slot]),
            remote(blk_s.at[slot, 1], sib_d.at[l, other], blk_send.at[slot], sd_recv.at[l, s], here.sibling),
        )

    def tile_loads(l, j, slot):
        cols = pl.ds(mult(j * TILE, TILE), TILE)
        pairs = [(d_ref.at[l, cols, :], wd_t.at[slot]), (p_ref.at[l, j], p_t.at[slot]), (q_ref.at[l, j], q_t.at[slot])]
        pairs += [(g_ref.at[l, m, :, cols], wgu_t.at[slot, :, pl.ds(m * TILE, TILE)]) for m in range(2)]
        return [pltpu.make_async_copy(src, dst, w_sem.at[slot, i]) for i, (src, dst) in enumerate(pairs)]

    def term_copies(l, j, slot):
        cols = pl.ds(mult(j * TILE, TILE), TILE)
        part = jnp.minimum(j // (C_PART // TILE), PAIRS - D_PAIRS - 1)
        own, sib = [], []
        for m in range(2):
            mine, other = term_s.at[slot, m, :, here.core], term_s.at[slot, m, :, 1 - here.core]
            own.append(pltpu.make_async_copy(mine, own_gu.at[l, m, :, :, cols], term_sem.at[slot, m]))
            to = sib_gu.at[l, m, :, :, cols]
            sib.append(remote(other, to, term_send.at[slot, m], sgu_recv.at[l, part], here.sibling))
        return own, sib

    def wait_terms(l, j, slot):
        own, sib = term_copies(l, j, slot)
        wait(own)
        for copy in sib:
            copy.wait_send()

    def wait_block(l, s, slot):
        own, sib = block_copies(l, s, slot)
        own.wait()
        sib.wait_send()

    def layer(i):
        l = 1 - i
        base = FIRST_EVENT + i * (PAIR_EVENTS + TILE_EVENTS)
        load_at = pltpu.make_async_copy(at_ref.at[l], at_s, misc_sem.at[0])
        load_at.start()
        pl.when(i == 0)(pltpu.make_async_copy(h1_ref, h_s, misc_sem.at[1]).start)
        pl.when(i == 1)(pltpu.make_async_copy(x_ref, h_s, misc_sem.at[1]).start)
        start(lhs_loads(l, 0, 0))
        start(tile_loads(l, 0, 0))

        def pair(s):
            slot = lax.rem(s, 2)
            pl.when(s < STEPS - 1)(lambda: start(lhs_loads(l, s + 1, 1 - slot)))
            wait(lhs_loads(l, s, slot))
            for b in range(2):
                blk_s[slot, b] = dot(lhs_t[slot, b], dh_s[...]).astype(BF16)
            start(block_copies(l, s, slot))
            pl.when(s >= 1)(lambda: wait_block(l, s - 1, 1 - slot))
            pl.when((i == 0) & (s == 1))(lambda: loop(FIRST_EVENT, FIRST_EVENT + AHEAD, fetch))

            def done_by(s):
                cap = jnp.where(i == 0, jnp.maximum(PLACES * s - 1, FIRST_EVENT), LAST_EVENT)
                return jnp.minimum(base + (PAIR_EVENTS * (s + 1)) // STEPS, cap)

            loop(jnp.where(s == 0, base, done_by(s - 1)), done_by(s), event)

        loop(0, STEPS, pair)
        wait_block(l, STEPS - 1, (STEPS - 1) % 2)
        load_at.wait()
        dacc[...] = jnp.zeros_like(dacc)

        def tick(j):
            slot = lax.rem(j, 2)
            pl.when(j + 1 < TILES)(lambda: start(tile_loads(l, j + 1, 1 - slot)))
            wait(tile_loads(l, j, slot))
            pl.when(j >= 2)(lambda: wait_terms(l, j - 2, slot))

            def done_by(j, half):
                cap = jnp.where(i == 0, PER_PAIR * (D_PAIRS + (j + 4) // (C_PART // TILE) - 1) - 1, LAST_EVENT)
                return jnp.minimum(base + PAIR_EVENTS + ((2 * j + half) * TILE_EVENTS) // (2 * TILES), cap)

            for r in range(ROW_CHUNKS):
                rows = pl.ds(r * ROWS, ROWS)
                dprod = dot(dh_s[rows, :], wd_t[slot], ((1,), (1,))).astype(BF16).astype(F32)
                dz_s[rows, pl.ds(0, TILE)] = (dprod * p_t[slot, rows, :]).astype(BF16)
                dz_s[rows, pl.ds(TILE, TILE)] = (dprod * q_t[slot, rows, :]).astype(BF16)
                dacc[rows, :] += dot(dz_s[rows, :], wgu_t[slot], ((1,), (1,)))
            loop(jnp.where(j == 0, base + PAIR_EVENTS, done_by(j - 1, 2)), done_by(j, 1), event)
            for r in range(2):
                term = dot(at_s[pl.ds(r * D // 2, D // 2), :], dz_s[...])
                for b in range(8):
                    for m in range(2):
                        block = term[b * RG : (b + 1) * RG, m * TILE : (m + 1) * TILE]
                        term_s[slot, m, r * 4 + b // 2, b % 2] = block.astype(BF16)
            own, sib = term_copies(l, j, slot)
            start(own + sib)
            loop(done_by(j, 1), done_by(j, 2), event)

        loop(0, TILES, tick)
        for j in (TILES - 2, TILES - 1):
            wait_terms(l, j, j % 2)
        pltpu.make_async_copy(h1_ref, h_s, misc_sem.at[1]).wait()

        def new_dh(r):
            rows = pl.ds(mult(r * CH, CH), CH)
            da = dacc[rows, :].astype(BF16).astype(F32)
            wide = h_s[rows, :].astype(F32)
            scale = lax.rsqrt(jnp.mean(wide * wide, -1, keepdims=True) + EPS)
            along = jnp.mean(da * wide, -1, keepdims=True) * scale * scale
            by_h = (scale * (da - wide * along)).astype(BF16).astype(F32)
            dh_s[rows, :] = (dh_s[rows, :].astype(F32) + by_h).astype(BF16)

        loop(0, T // CH, new_dh)

    load_dy = pltpu.make_async_copy(dy_ref, dh_s, misc_sem.at[2])
    load_dy.start()
    load_dy.wait()
    loop(0, LAYERS, layer)
    put_dx = pltpu.make_async_copy(dh_s, dx_out, misc_sem.at[2])
    put_dx.start()
    loop(FIRST_EVENT + LAYERS * (PAIR_EVENTS + TILE_EVENTS), LAST_EVENT, event)
    loop(LAST_EVENT - LAG, LAST_EVENT, lambda e: with_lane(e, Lane.wait_out))
    put_dx.wait()


def backward(dy, x, h1, gathered_gu, gathered_d, p, q, actt, at):
    any_ = pl.BlockSpec(memory_space=pl.ANY)
    vmem, dma = pltpu.VMEM, pltpu.SemaphoreType.DMA
    terms_gu = jax.ShapeDtypeStruct((LAYERS, 2, 8, RG, FFP), BF16)
    terms_d = jax.ShapeDtypeStruct((LAYERS, 8, RD, D), BF16)
    two = (2, 2)
    per_part = (LAYERS, PAIRS, 2)
    outs = (
        jax.ShapeDtypeStruct((T, D), BF16),
        jax.ShapeDtypeStruct((2, LAYERS, RG, FF), BF16),
        jax.ShapeDtypeStruct((LAYERS, RD, D), BF16),
        terms_gu, terms_gu, terms_d, terms_d,
    )
    return pl.pallas_call(
        backward_kernel,
        out_shape=outs,
        in_specs=[any_] * 9,
        out_specs=(any_,) * len(outs),
        scratch_shapes=[
            vmem((T, D), BF16),
            vmem((D, T), BF16),
            vmem((T, D), BF16),
            vmem((T, D), F32),
            vmem((*two, RD, T), BF16),
            vmem((*two, RD, D), BF16),
            vmem((2, D, 2 * TILE), BF16),
            vmem((2, TILE, D), BF16),
            vmem((2, T, TILE), F32),
            vmem((2, T, TILE), F32),
            vmem((T, 2 * TILE), BF16),
            vmem((*two, 8, 2, RG, TILE), BF16),
            vmem((D_PAIRS, 2, STEPS, D_LAST, D), BF16),
            vmem((PAIRS - D_PAIRS, 2, STEPS, RG, C_PART), BF16),
            vmem((PLACES, 2, D_LAST, D), BF16),
            vmem((PLACES, 2, RG, C_PART), BF16),
            dma((*per_part, STEPS)),
            dma((*per_part, STEPS)),
            dma((PLACES, 2)),
            dma(per_part),
            dma((LAYERS, STEPS)),
            dma((LAYERS, PAIRS - D_PAIRS)),
            dma(two),
            dma((2,)),
            dma((2,)),
            dma((2, 5)),
            dma(two),
            dma(two),
            dma((3,)),
        ],
        compiler_params=pltpu.CompilerParams(
            collective_id=1, has_side_effects=True, vmem_limit_bytes=63 * 1024 * 1024
        ),
        name="backward_reduce",
    )(dy, x, h1, gathered_gu, gathered_d, p, q, actt, at)


def solution(mesh):
    def step(x, dy, wg, wu, wd):
        gu, d, p, q, actt, at, h1 = forward(x[0], wg, wu, wd)
        dx, dgu, dd, *_ = backward(dy[0], x[0], h1, gu, d, p, q, actt, at)
        return dx[None], dgu[0], dgu[1], dd

    both, rows = P(("rep", "dp"), None, None), P(None, "dp", None)
    own = P("rep", "dp", None)
    return jax.shard_map(
        step,
        mesh=mesh,
        in_specs=(both, both, rows, rows, rows),
        out_specs=(both, own, own, own),
        check_vma=False,
    )
```

```python
import functools

import jax
import jax.numpy as jnp
from jax import lax
from jax.experimental import pallas as pl
from jax.experimental.pallas import tpu as pltpu
from jax.sharding import PartitionSpec as P

MESH = pl.DeviceIdType.MESH
BF16, F32 = jnp.bfloat16, jnp.float32
LAYERS, T, D, FF = 2, 1024, 896, 4736
N = 16
TILE = 256
TILES = 19
FFP = TILE * TILES
RG, RD = D // N, FF // N
EPS = 1e-6
CH = 128
ROW_CHUNKS = 2
ROWS = T // ROW_CHUNKS

DOWN = 2
COLUMNS = {0: (0, 10), 1: (10, TILES)}
GU_A = {0: 7 * 128, 1: 5 * 128}
UNIT_KINDS = (0, 1, DOWN, 0, 1, DOWN)
UNITS, HOPS, ITEMS = len(UNIT_KINDS), 7, 2
LAYER_1 = 3
D_A = 96
D_B = RD - 2 * D_A
STAGGER = 4
PER_UNIT = STAGGER * 2 * ITEMS
READY = 2 * PER_UNIT + 1
N_PIECES = ((0, 512), (512, 384))


class Place:
    def __init__(self):
        self.rep = lax.axis_index("rep")
        me = lax.axis_index("dp")
        self.core = lax.rem(me, 2)
        self.chip = me // 2
        self.ring = jnp.where(self.chip < 4, self.chip, 11 - self.chip)
        self.way = 1 - 2 * self.core
        self.next = (self.rep, self.device(1))
        self.prev = (self.rep, self.device(-1))
        self.sibling = (self.rep, self.chip * 2 + 1 - self.core)
        self.other = (1 - self.rep, me)

    def chip_at(self, steps):
        r = lax.rem(self.ring + self.way * steps + 16, 8)
        return jnp.where(r < 4, r, 11 - r)

    def device(self, steps):
        return self.chip_at(steps) * 2 + self.core


def barrier(devices):
    sem = pltpu.get_barrier_semaphore()
    for device in devices:
        pl.semaphore_signal(sem, inc=1, device_id=device, device_id_type=MESH)
    pl.semaphore_wait(sem, len(devices))


def remote(src, dst, send, recv, device):
    return pltpu.make_async_remote_copy(
        src_ref=src, dst_ref=dst, send_sem=send, recv_sem=recv, device_id=device, device_id_type=MESH
    )


def loop(lo, hi, body):
    def run(i, carry):
        body(i)
        return carry

    lax.fori_loop(lo, hi, run, 0)


def start(copies):
    for copy in copies:
        copy.start()


def wait(copies):
    for copy in copies:
        copy.wait()


def mult(x, m):
    return pl.multiple_of(x, m)


def dot(a, b, dims=((1,), (0,))):
    return lax.dot_general(a, b, (dims, ((), ())), preferred_element_type=F32)


class Gather:
    def __init__(self, here, sources, g_out, d_out, sems):
        self.here, self.sources, self.g_out, self.d_out = here, sources, g_out, d_out
        self.ring_recv, self.x_recv, self.sib_recv, self.ring_send, self.x_send, self.sib_send = sems

    @staticmethod
    def columns(kind):
        first, end = COLUMNS[kind]
        return first * TILE, min(end * TILE, FF) - first * TILE

    def cut(self, kind, is_own, group):
        if kind == DOWN:
            return (pl.ds(mult(D_B + D_A * group, 8), D_A) if is_own else pl.ds(0, D_B)), pl.ds(0, D)
        first, size = self.columns(kind)
        common = size - 2 * GU_A[kind]
        if is_own:
            return pl.ds(0, RG), pl.ds(mult(first + common + GU_A[kind] * group, 128), GU_A[kind])
        return pl.ds(0, RG), pl.ds(first, common)

    def region(self, l, kind, dev, is_own, group):
        rows, cols = self.cut(kind, is_own, group)
        if kind == DOWN:
            return self.d_out.at[l, pl.ds(mult(dev * RD + rows.start, 8), rows.size), cols]
        return self.g_out.at[l, :, pl.ds(mult(dev * RG, 8), RG), cols]

    def send_ring(self, src, dst, u, t, item):
        return remote(src, dst, self.ring_send.at[u], self.ring_recv.at[u, t - 1, item], self.here.next)

    def send_x(self, reg, u, t):
        return remote(reg, reg, self.x_send.at[u], self.x_recv.at[u, t - 1], self.here.other)

    def send_sibling(self, src, dst, u):
        return remote(src, dst, self.sib_send.at[u], self.sib_recv.at[u], self.here.sibling)

    def start_own(self, u, l, kind):
        me = self.here.device(0)
        sources = [ref.at[l] for ref in (self.sources[2:] if kind == DOWN else self.sources[:2])]
        for item in range(ITEMS):
            rows, cols = self.cut(kind, item == 0, self.here.rep)
            to = self.region(l, kind, me, item == 0, self.here.rep)
            for m, src in enumerate(sources):
                self.send_ring(src.at[rows, cols], to if kind == DOWN else to.at[m], u, 1, item).start()
        for m, src in enumerate(sources):
            if kind == DOWN:
                self.send_sibling(src, self.d_out.at[l, pl.ds(mult(me * RD, 8), RD), :], u).start()
            else:
                cols = pl.ds(*self.columns(kind))
                to = self.g_out.at[l, m, pl.ds(mult(me * RG, 8), RG), cols]
                self.send_sibling(src.at[:, cols], to, u).start()

    def ring_event(self, u, l, kind, t, item):
        is_own = item == 0
        reg = self.region(l, kind, self.here.device(-t), is_own, self.here.rep)
        self.send_ring(reg, reg, u, t, item).wait_recv()
        pl.when(t < HOPS)(lambda: self.send_ring(reg, reg, u, t + 1, item).start())
        if is_own:
            self.send_x(reg, u, t).start()
        self.send_sibling(reg, reg, u).start()

    def x_event(self, u, l, kind, t):
        reg = self.region(l, kind, self.here.device(-t), True, 1 - self.here.rep)
        self.send_x(reg, u, t).wait_recv()
        self.send_sibling(reg, reg, u).start()

    def event(self, e):
        round_, place = e // (2 * ITEMS), lax.rem(e, 2 * ITEMS)
        newer, item = place // ITEMS, lax.rem(place, ITEMS)

        def at(round_):
            return (round_ + STAGGER) // STAGGER - 2 + newer, lax.rem(round_, STAGGER) + STAGGER * (1 - newer)

        def of_kind(u, kind):
            first, *others = [i for i in range(UNITS) if UNIT_KINDS[i] == kind]
            return functools.reduce(lambda so_far, i: so_far | (u == i), others, u == first)

        u, t = at(round_)
        l = jnp.where(u < LAYER_1, 0, 1)
        was, hop = at(round_ - 1)
        was_l = jnp.where(was < LAYER_1, 0, 1)
        crosses = (item == 0) & (hop > 0) & (round_ > 0)
        for kind in sorted(set(UNIT_KINDS)):

            @pl.when(of_kind(u, kind))
            def _(kind=kind):
                pl.when((t == 0) & (item == 0))(functools.partial(self.start_own, u, l, kind))
                for i in range(ITEMS):
                    pl.when((t > 0) & (item == i))(functools.partial(self.ring_event, u, l, kind, t, i))

            pl.when(crosses & of_kind(was, kind))(functools.partial(self.x_event, was, was_l, kind, hop))

    def events(self, lo, hi):
        loop(lo, hi, self.event)

    def whole(self, l, kind, of_gu, of_d):
        if kind == DOWN:
            return self.d_out.at[l, pl.ds(0, of_d), :]
        rows, width = of_gu
        return self.g_out.at[l, :, pl.ds(0, rows), pl.ds(0, width)]

    def wait_unit(self, u):
        kind, l = UNIT_KINDS[u], int(u >= LAYER_1)
        width = 0 if kind == DOWN else self.columns(kind)[1]
        half = self.whole(l, kind, (D // 2, width), FF // 2)
        self.send_sibling(half, half, u).wait_recv()

    def wait_sends(self, u):
        kind, l = UNIT_KINDS[u], int(u >= LAYER_1)
        width, own = (0, 0) if kind == DOWN else (self.columns(kind)[1], GU_A[kind])
        sent = (
            self.whole(l, kind, (HOPS * RG, width - own), HOPS * (D_A + D_B)),
            self.whole(l, kind, (HOPS * RG, own), HOPS * D_A),
            self.whole(l, kind, (D // 2, width), FF // 2),
        )
        for ref, sem in zip(sent, (self.ring_send, self.x_send, self.sib_send)):
            remote(ref, ref, sem.at[u], sem.at[u], self.here.next).wait_send()


def along(k, points):
    out = points[-1][1]
    for (k0, e0), (k1, e1) in reversed(list(zip(points, points[1:]))):
        out = jnp.where(k < k1, e0 + (k - k0) * (e1 - e0) // (k1 - k0), out)
    return out


TILE_POINTS = (
    ((0, 0), (20, PER_UNIT), (2 * TILES, 2 * PER_UNIT)),
    ((0, 3 * PER_UNIT), (20, 4 * PER_UNIT), (2 * TILES, 4 * PER_UNIT + 12)),
)
FORWARD_END = READY + TILE_POINTS[1][-1][1]
GATHER_END = READY + (UNITS - 1) * PER_UNIT


def forward_pass(
    here, gather, x_ref, g_out, d_out, p_out, q_out, actt_out, at_out, h1_out, local_sem, w_sem, o_sem, wd_sem, at_sem,
    a_s, h_s, at_s, prod_s, wd_s, wgu_t, p_s, q_s, pt_s, zc, zr,
):
    load_x = pltpu.make_async_copy(x_ref, h_s, at_sem.at[0])
    load_x.start()
    gather.events(ITEMS, 2 * ITEMS)
    zc[...] = jnp.zeros_like(zc)
    zr[...] = jnp.zeros_like(zr)
    me = here.device(0)
    wg_ref, wu_ref, wd_ref = gather.sources
    locals_ = []
    for l in range(LAYERS):
        for m in range(2):
            locals_.append((zc, g_out.at[l, m, :, pl.ds(FF, FFP - FF)]))
            locals_.append(((wg_ref, wu_ref)[m].at[l], g_out.at[l, m, pl.ds(mult(me * RG, 8), RG), pl.ds(0, FF)]))
        locals_.append((zr, d_out.at[l, pl.ds(FF, FFP - FF), :]))
        locals_.append((wd_ref.at[l], d_out.at[l, pl.ds(mult(me * RD, 8), RD), :]))
    locals_ = [pltpu.make_async_copy(src, dst, local_sem.at[i]) for i, (src, dst) in enumerate(locals_)]
    start(locals_)
    load_x.wait()

    def put_at(l):
        return pltpu.make_async_copy(at_s, at_out.at[l], at_sem.at[0])

    put_h = pltpu.make_async_copy(h_s, h1_out, at_sem.at[1])

    def norm(l, first_event, count):
        def chunk(i):
            rows = pl.ds(mult(i * CH, CH), CH)
            wide = h_s[rows, :].astype(F32)
            a = (wide * lax.rsqrt(jnp.mean(wide * wide, -1, keepdims=True) + EPS)).astype(BF16)
            a_s[rows, :] = a
            at_s[:, rows] = a.T
            gather.events(first_event + i * count, first_event + (i + 1) * count)

        loop(0, T // CH, chunk)
        put_at(l).start()

    def add_mlp(first_event):
        parts = [
            pltpu.make_async_copy(d_out.at[0, :, pl.ds(*piece)], wd_s.at[:, pl.ds(*piece)], wd_sem.at[i])
            for i, piece in enumerate(N_PIECES)
        ]
        start(parts)
        for i, piece in enumerate(N_PIECES):
            parts[i].wait()
            cols = pl.ds(*piece)

            def rows_part(r):
                rows = pl.ds(mult(r * ROWS, ROWS), ROWS)
                y = dot(prod_s[rows, :], wd_s[:, cols]).astype(BF16).astype(F32)
                h_s[rows, cols] = (h_s[rows, cols].astype(F32) + y).astype(BF16)
                now = first_event + (i * ROW_CHUNKS + r) * ITEMS
                gather.events(now, now + ITEMS)

            loop(0, ROW_CHUNKS, rows_part)

    def layer(l):
        def loads(j, slot):
            cols = pl.ds(mult(j * TILE, TILE), TILE)
            return [
                pltpu.make_async_copy(
                    g_out.at[l, m, :, cols], wgu_t.at[slot, :, pl.ds(m * TILE, TILE)], w_sem.at[slot, m]
                )
                for m in range(2)
            ]

        def stores(j, slot):
            rows = pl.ds(mult(j * TILE, TILE), TILE)
            pairs = ((p_s, p_out.at[l, j]), (q_s, q_out.at[l, j]), (pt_s, actt_out.at[l, rows, :]))
            return [pltpu.make_async_copy(src.at[slot], dst, o_sem.at[slot, i]) for i, (src, dst) in enumerate(pairs)]

        def done_by(k):
            return READY + jnp.where(l == 0, along(k, TILE_POINTS[0]), along(k, TILE_POINTS[1]))

        firsts = {u: COLUMNS[kind][0] for u, kind in enumerate(UNIT_KINDS) if kind != DOWN}

        def tick(j):
            slot = lax.rem(j, 2)
            for u, first in firsts.items():

                @pl.when((j == first) & ((l == 0) == (u < LAYER_1)))
                def _(u=u):
                    gather.wait_unit(u)

            is_first, next_is_first = ((k == 0) | (k == COLUMNS[1][0]) for k in (j, j + 1))
            pl.when(is_first)(lambda: start(loads(j, slot)))
            pl.when((j + 1 < TILES) & ~next_is_first)(lambda: start(loads(j + 1, 1 - slot)))
            wait(loads(j, slot))
            pl.when(j >= 2)(lambda: wait(stores(j - 2, slot)))

            def row_chunk(r):
                rows = pl.ds(mult(r * ROWS, ROWS), ROWS)
                both = dot(a_s[rows, :], wgu_t[slot])
                gate, up = both[:, :TILE], both[:, TILE:]
                s = 0.5 * jnp.tanh(0.5 * gate) + 0.5
                q = gate * s
                q_s[slot, rows, :] = q
                p_s[slot, rows, :] = up * (s + q * (1 - s))
                prod = (q * up).astype(BF16)
                pt_s[slot, :, rows] = prod.T
                prod_s[rows, pl.ds(mult(j * TILE, TILE), TILE)] = prod
                gather.events(done_by(2 * j + r), done_by(2 * j + r + 1))

            loop(0, ROW_CHUNKS, row_chunk)
            start(stores(j, slot))

        loop(0, TILES, tick)
        for j in (TILES - 2, TILES - 1):
            wait(stores(j, j % 2))

        @pl.when(l == 0)
        def _():
            gather.wait_unit(UNIT_KINDS.index(DOWN))
            now = READY + 2 * PER_UNIT
            put_at(0).wait()
            add_mlp(now)
            now += ITEMS * ROW_CHUNKS * len(N_PIECES)
            norm(1, now, 1)
            put_h.start()

    norm(0, 2 * ITEMS, 1)
    gather.events(2 * ITEMS + T // CH, READY)
    wait(locals_)
    loop(0, LAYERS, layer)
    put_h.wait()
    put_at(1).wait()


PAIRS, STEPS, PLACES = 4, 8, 4
PER_PAIR = STEPS // 2 * PLACES
QUEUE = LAYERS * PAIRS + 1
SECOND = PAIRS + 1
D_PARTS = ((0, 152), (152, 144))
BIG = 2 * TILE
BIGS = (TILES + 1) // 2
PART_BIGS = 3
C_PART = PART_BIGS * BIG
C_LAST = FF - 2 * C_PART
LAST_EVENT = (QUEUE + 1) * PER_PAIR
AHEAD = PLACES - 1
LAG = 2 * PLACES
BEFORE, BETWEEN, AFTER = (2, 63), (12, 74), (63, 120)


def backward_pass(
    here, gather, dy_ref, x_ref, h1_ref, g_ref, d_ref, p_ref, q_ref, actt_ref, at_ref,
    dx_out, dg_out, du_out, dd_out, own_gu, sib_gu, own_d, sib_d, slot_d, slot_c,
    red_recv, red_send, st_sem, fin_sem, sd_recv, sgu_recv, lhs_sem, blk_sem, blk_send, w_sem, term_sem, term_send, misc_sem,
    dh_s, at_s, h_s, dacc, lhs_t, blk_s, wgu_t, wd_t, p_t, q_t, dz_s, term_s, st_d, st_c,
):
    def chips(s):
        return here.chip_at(-1 - s), here.chip_at(1 + s)

    class Lane:
        def __init__(self, l, pair, lane, s, place, down, last):
            chip, _ = chips(s)
            self.s, self.place, self.lane = s, place, lane
            self.sems = [sem.at[l, pair, lane] for sem in (red_recv, red_send)]
            self.fin = fin_sem.at[l, pair, lane]
            if down:
                first, size = D_PARTS[last]
                rows, cut = pl.ds(first, size), pl.ds(0, size)
                self.slots = [slot_d.at[lane, to, cut, :] for to in (s, s + 1)]
                self.st = [st_d.at[place, i, cut, :] for i in range(2)]
                self.terms = [ref.at[l, chip, rows, :] for ref in (own_d, sib_d)]
                self.result = dd_out.at[l, rows, :]
            else:
                part = pair - 1
                cols, cut = (pl.ds(first, C_LAST if last else C_PART) for first in (mult(part * C_PART, 128), 0))
                self.slots = [slot_c.at[part, lane, to, :, cut] for to in (s, s + 1)]
                self.st = [st_c.at[place, i, :, cut] for i in range(2)]
                self.terms = [ref.at[l, lane, chip, :, cols] for ref in (own_gu, sib_gu)]
                self.result = [out.at[l, :, cols] for out in (dg_out, du_out)]

        def stage(self):
            pairs = zip(self.terms, self.st)
            return [pltpu.make_async_copy(a, b, st_sem.at[self.place, i]) for i, (a, b) in enumerate(pairs)]

        def send(self, to):
            recv, sent = self.sems
            return remote(self.slots[0], self.slots[to], sent.at[self.s], recv.at[self.s + to], here.next)

        def finish(self, action):
            if not isinstance(self.result, list):
                action(pltpu.make_async_copy(self.slots[0], self.result, self.fin))
                return
            for lane, result in enumerate(self.result):
                copy = pltpu.make_async_copy(self.slots[0], result, self.fin)
                pl.when(self.lane == lane)(functools.partial(action, copy))

        def step(self):
            wait(self.stage())
            slot = self.slots[0]
            ends = [st[...].astype(F32) for st in self.st]

            @pl.when(self.s > 0)
            def _():
                self.send(0).wait_recv()
                slot[...] = (slot[...].astype(F32) + (ends[0] + ends[1])).astype(BF16)

            @pl.when(self.s == 0)
            def _():
                slot[...] = (ends[0] + ends[1]).astype(BF16)

            pl.when(self.s < STEPS - 1)(lambda: self.send(1).start())
            pl.when(self.s == STEPS - 1)(lambda: self.finish(lambda copy: copy.start()))

        def wait_out(self):
            pl.when(self.s < STEPS - 1)(lambda: self.send(1).wait_send())
            pl.when(self.s == STEPS - 1)(lambda: self.finish(lambda copy: copy.wait()))

        def prefetch(self):
            start(self.stage())

    def with_lane(e, action, ahead_of=lambda l, pair, lane, s: None):
        round_, place = e // PLACES, lax.rem(e, PLACES)
        new = place // 2
        index = round_ // PLACES + new - 1
        s = lax.rem(round_, PLACES) + PLACES * (1 - new)
        lane = lax.rem(place, 2)

        @pl.when((index >= 0) & (index < QUEUE) & (index != 1))
        def _():
            second = jnp.where(index < SECOND, 0, 1)
            free = jnp.where((index > 1) & (index < SECOND), 1, 0)
            l, pair = 1 - second, index - SECOND * second - free
            ahead_of(l, pair, lane, s)
            for is_down, is_last, chosen in (
                (True, False, (pair == 0) & (lane == 0)), (True, True, (pair == 0) & (lane == 1)),
                (False, False, (pair > 0) & (pair < PAIRS - 1)), (False, True, pair == PAIRS - 1),
            ):
                pl.when(chosen)(lambda: action(Lane(l, pair, lane, s, place, is_down, is_last)))

    def terms_ready(l, pair, lane, s):
        @pl.when((pair == 0) & (lane == 0))
        def _():
            whole = sib_d.at[l, 0]
            remote(whole, whole, blk_send.at[0], sd_recv.at[l, s], here.sibling).wait_recv()

        @pl.when((pair > 0) & (lane == 0) & (s == 0))
        def _():
            for is_last in (False, True):
                width = FFP - 2 * C_PART if is_last else C_PART

                @pl.when((pair == PAIRS - 1) == is_last)
                def _(width=width):
                    part = sib_gu.at[l, :, :, :, pl.ds(0, width)]
                    sem = sgu_recv.at[l, pair - 1]
                    remote(part, part, term_send.at[0, 0], sem, here.sibling).wait_recv()

    def events(lo, hi):
        loop(lo, hi, event)

    def fetch(e):
        with_lane(e, Lane.prefetch, terms_ready)

    def event(e):
        pl.when(e >= LAG)(lambda: with_lane(e - LAG, Lane.wait_out))
        fetch(e + AHEAD)
        with_lane(e, Lane.step)

    def lhs_loads(l, s, slot):
        mine, other = chips(s)
        rows = ((mine * 2 + here.core) * RD, (other * 2 + 1 - here.core) * RD)
        return [
            pltpu.make_async_copy(actt_ref.at[l, pl.ds(mult(row, 8), RD), :], lhs_t.at[slot, i], lhs_sem.at[slot, i])
            for i, row in enumerate(rows)
        ]

    def block_copies(l, s, slot):
        mine, other = chips(s)
        return (
            pltpu.make_async_copy(blk_s.at[slot, 0], own_d.at[l, mine], blk_sem.at[slot]),
            remote(blk_s.at[slot, 1], sib_d.at[l, other], blk_send.at[slot], sd_recv.at[l, s], here.sibling),
        )

    def both_halves(j, action):
        action(0)
        pl.when(j < BIGS - 1)(lambda: action(1))

    def tile_loads(l, j, slot, half):
        tile = 2 * j + half
        src = pl.ds(mult(tile * TILE, TILE), TILE)
        dst = pl.ds(half * TILE, TILE)
        pairs = [
            (d_ref.at[l, src, :], wd_t.at[slot, dst, :]),
            (p_ref.at[l, tile], p_t.at[slot, :, dst]),
            (q_ref.at[l, tile], q_t.at[slot, :, dst]),
        ]
        pairs += [(g_ref.at[l, m, :, src], wgu_t.at[slot, :, pl.ds((2 * half + m) * TILE, TILE)]) for m in range(2)]
        return [pltpu.make_async_copy(src, dst, w_sem.at[slot, half, i]) for i, (src, dst) in enumerate(pairs)]

    def term_copies(l, j, half):
        cols = pl.ds(mult((2 * j + half) * TILE, TILE), TILE)
        part = jnp.minimum(j // PART_BIGS, PAIRS - 2)
        own, sib = [], []
        for m in range(2):
            mine, other = term_s.at[half, m, :, here.core], term_s.at[half, m, :, 1 - here.core]
            own.append(pltpu.make_async_copy(mine, own_gu.at[l, m, :, :, cols], term_sem.at[half, m]))
            to = sib_gu.at[l, m, :, :, cols]
            sib.append(remote(other, to, term_send.at[half, m], sgu_recv.at[l, part], here.sibling))
        return own, sib

    def start_terms(l, j, half):
        own, sib = term_copies(l, j, half)
        start(own + sib)

    def wait_terms(l, j, half):
        own, sib = term_copies(l, j, half)
        wait(own)
        for copy in sib:
            copy.wait_send()

    def wait_block(l, s, slot):
        own, sib = block_copies(l, s, slot)
        own.wait()
        sib.wait_send()

    def layer(i):
        l = 1 - i
        before, between, after = (jnp.where(i == 0, *counts) for counts in (BEFORE, BETWEEN, AFTER))
        load_at = pltpu.make_async_copy(at_ref.at[l], at_s, misc_sem.at[0])
        load_at.start()
        pl.when(i == 0)(pltpu.make_async_copy(h1_ref, h_s, misc_sem.at[1]).start)
        pl.when(i == 1)(pltpu.make_async_copy(x_ref, h_s, misc_sem.at[1]).start)
        start(lhs_loads(l, 0, 0))
        first_loads = lambda: both_halves(0, lambda half: start(tile_loads(l, 0, 0, half)))
        pl.when(i == 1)(first_loads)

        def pair(s):
            slot = lax.rem(s, 2)
            pl.when(s < STEPS - 1)(lambda: start(lhs_loads(l, s + 1, 1 - slot)))
            wait(lhs_loads(l, s, slot))
            for b in range(2):
                blk_s[slot, b] = dot(lhs_t[slot, b], dh_s[...]).astype(BF16)
            start(block_copies(l, s, slot))

            @pl.when(i == 0)
            def _():
                lo, hi = (FORWARD_END + (GATHER_END - FORWARD_END) * to // STEPS for to in (s, s + 1))
                gather.events(lo, hi)

            pl.when(s >= 1)(lambda: wait_block(l, s - 1, 1 - slot))
            pl.when((i == 0) & (s == 1))(lambda: loop(BEFORE[0], BEFORE[0] + AHEAD, fetch))

            def done_by(s):
                cap = jnp.where(i == 0, jnp.maximum(PLACES * s - 1, before), LAST_EVENT)
                return jnp.minimum(before + ((between - before) * (s + 1)) // STEPS, cap)

            loop(jnp.where(s == 0, before, done_by(s - 1)), done_by(s), event)

        loop(0, STEPS, pair)
        wait_block(l, STEPS - 1, (STEPS - 1) % 2)

        @pl.when(i == 0)
        def _():
            gather.wait_unit(UNITS - 1)
            first_loads()

        load_at.wait()
        dacc[...] = jnp.zeros_like(dacc)

        def tick(j):
            slot = lax.rem(j, 2)
            pl.when(j + 1 < BIGS)(lambda: both_halves(j + 1, lambda half: start(tile_loads(l, j + 1, 1 - slot, half))))
            both_halves(j, lambda half: wait(tile_loads(l, j, slot, half)))

            @pl.when(j == BIGS - 1)
            def _():
                for ref in (p_t, q_t):
                    ref[slot, :, pl.ds(TILE, TILE)] = jnp.zeros((T, TILE), F32)

            def done_by(k):
                ready = jnp.maximum(k - 2, 0) // (PART_BIGS * 4)
                cap = jnp.where(i == 0, PER_PAIR * (2 + jnp.minimum(ready, PAIRS - 2)) - 1, LAST_EVENT)
                return jnp.minimum(between + (k * (after - between)) // (4 * BIGS), cap)

            def quarter(k):
                events(done_by(4 * j + k), done_by(4 * j + k + 1))

            for r in range(2):
                rows = pl.ds(r * ROWS, ROWS)
                dprod = dot(dh_s[rows, :], wd_t[slot], ((1,), (1,))).astype(BF16).astype(F32)
                by_gate = (dprod * p_t[slot, rows, :]).astype(BF16)
                by_up = (dprod * q_t[slot, rows, :]).astype(BF16)
                for half in range(2):
                    for m, by in enumerate((by_gate, by_up)):
                        part = by[:, half * TILE : (half + 1) * TILE]
                        dz_s[rows, pl.ds((2 * half + m) * TILE, TILE)] = part
                dacc[rows, :] += dot(dz_s[rows, :], wgu_t[slot], ((1,), (1,)))
                if r == 1:
                    pl.when(j > 0)(lambda: [wait_terms(l, j - 1, half) for half in range(2)] and None)
                quarter(r)
            for r in range(2):
                term = dot(at_s[pl.ds(r * D // 2, D // 2), :], dz_s[...])
                for b in range(8):
                    for half in range(2):
                        for m in range(2):
                            col = (2 * half + m) * TILE
                            block = term[b * RG : (b + 1) * RG, col : col + TILE]
                            term_s[half, m, r * 4 + b // 2, b % 2] = block.astype(BF16)
                if r == 1:
                    both_halves(j, lambda half: start_terms(l, j, half))
                quarter(2 + r)

        loop(0, BIGS, tick)
        wait_terms(l, BIGS - 1, 0)
        pltpu.make_async_copy(h1_ref, h_s, misc_sem.at[1]).wait()

        def new_dh(r):
            rows = pl.ds(mult(r * CH, CH), CH)
            da = dacc[rows, :].astype(BF16).astype(F32)
            wide = h_s[rows, :].astype(F32)
            scale = lax.rsqrt(jnp.mean(wide * wide, -1, keepdims=True) + EPS)
            along = jnp.mean(da * wide, -1, keepdims=True) * scale * scale
            by_h = (scale * (da - wide * along)).astype(BF16).astype(F32)
            dh_s[rows, :] = (dh_s[rows, :].astype(F32) + by_h).astype(BF16)

        loop(0, T // CH, new_dh)

    load_dy = pltpu.make_async_copy(dy_ref, dh_s, misc_sem.at[2])
    load_dy.start()
    load_dy.wait()
    loop(0, LAYERS, layer)
    put_dx = pltpu.make_async_copy(dh_s, dx_out, misc_sem.at[2])
    put_dx.start()
    loop(AFTER[1], LAST_EVENT, event)
    loop(LAST_EVENT - LAG, LAST_EVENT, lambda e: with_lane(e, Lane.wait_out))
    put_dx.wait()


def kernel(
    dy_ref, x_ref, wg_ref, wu_ref, wd_ref,
    dx_out, dg_out, du_out, dd_out, own_gu, sib_gu, own_d, sib_d, g_out, d_out, p_out, q_out, actt_out, at_out, h1_out,
    slot_d, slot_c, *sems,
):
    gather_sems, forward_sems, backward_sems = sems[:6], sems[6:11], sems[11:]
    here = Place()
    barrier((here.next, here.prev, here.sibling, here.other))
    gather = Gather(here, (wg_ref, wu_ref, wd_ref), g_out, d_out, gather_sems)
    vmem = pltpu.VMEM
    two = (2, 2)
    pl.run_scoped(
        functools.partial(
            forward_pass, here, gather, x_ref, g_out, d_out, p_out, q_out, actt_out, at_out, h1_out, *forward_sems
        ),
        vmem((T, D), BF16),
        vmem((T, D), BF16),
        vmem((D, T), BF16),
        vmem((T, FFP), BF16),
        vmem((FFP, D), BF16),
        vmem((2, D, 2 * TILE), BF16),
        vmem((2, T, TILE), F32),
        vmem((2, T, TILE), F32),
        vmem((2, TILE, T), BF16),
        vmem((D, FFP - FF), BF16),
        vmem((FFP - FF, D), BF16),
    )
    pl.run_scoped(
        functools.partial(
            backward_pass, here, gather, dy_ref, x_ref, h1_out, g_out, d_out, p_out, q_out, actt_out, at_out,
            dx_out, dg_out, du_out, dd_out, own_gu, sib_gu, own_d, sib_d, slot_d, slot_c, *backward_sems,
        ),
        vmem((T, D), BF16),
        vmem((D, T), BF16),
        vmem((T, D), BF16),
        vmem((T, D), F32),
        vmem((*two, RD, T), BF16),
        vmem((*two, RD, D), BF16),
        vmem((2, D, 2 * BIG), BF16),
        vmem((2, BIG, D), BF16),
        vmem((2, T, BIG), F32),
        vmem((2, T, BIG), F32),
        vmem((T, 2 * BIG), BF16),
        vmem((*two, 8, 2, RG, TILE), BF16),
        vmem((PLACES, 2, D_PARTS[0][1], D), BF16),
        vmem((PLACES, 2, RG, C_LAST), BF16),
    )
    for u in range(UNITS):
        gather.wait_sends(u)


def both_passes(dy, x, wg, wu, wd):
    any_, vmem = pl.BlockSpec(memory_space=pl.ANY), pl.BlockSpec(memory_space=pltpu.VMEM)
    dma = pltpu.SemaphoreType.DMA
    shape = jax.ShapeDtypeStruct
    two = (2, 2)
    per_part = (LAYERS, PAIRS, 2)
    outs = (
        shape((T, D), BF16),
        *[shape((LAYERS, RG, FF), BF16)] * 2,
        shape((LAYERS, RD, D), BF16),
        *[shape((LAYERS, 2, 8, RG, FFP), BF16)] * 2,
        *[shape((LAYERS, 8, RD, D), BF16)] * 2,
        shape((LAYERS, 2, D, FFP), BF16),
        shape((LAYERS, FFP, D), BF16),
        *[shape((LAYERS, TILES, T, TILE), F32)] * 2,
        shape((LAYERS, FFP, T), BF16),
        shape((LAYERS, D, T), BF16),
        shape((T, D), BF16),
    )
    gather_sems = [dma((UNITS, HOPS, ITEMS)), dma((UNITS, HOPS)), *[dma((UNITS,))] * 4]
    forward_sems = [dma((LAYERS * 6,)), dma(two), dma((2, 3)), dma((2,)), dma((2,))]
    backward_sems = [
        dma((*per_part, STEPS)),
        dma((*per_part, STEPS)),
        dma((PLACES, 2)),
        dma(per_part),
        dma((LAYERS, STEPS)),
        dma((LAYERS, PAIRS - 1)),
        dma(two),
        dma((2,)),
        dma((2,)),
        dma((*two, 5)),
        dma(two),
        dma(two),
        dma((3,)),
    ]
    return pl.pallas_call(
        kernel,
        out_shape=outs,
        in_specs=[any_] * 2 + [vmem] * 3,
        out_specs=(any_,) * len(outs),
        scratch_shapes=[
            pltpu.VMEM((2, STEPS, D_PARTS[0][1], D), BF16),
            pltpu.VMEM((PAIRS - 1, 2, STEPS, RG, C_LAST), BF16),
            *gather_sems,
            *forward_sems,
            *backward_sems,
        ],
        compiler_params=pltpu.CompilerParams(
            collective_id=0, has_side_effects=True, vmem_limit_bytes=63 * 1024 * 1024
        ),
        name="both_passes",
    )(dy, x, wg, wu, wd)


def solution(mesh):
    def step(x, dy, wg, wu, wd):
        dx, dg, du, dd, *_ = both_passes(dy[0], x[0], wg, wu, wd)
        return dx[None], dg, du, dd

    both, rows = P(("rep", "dp"), None, None), P(None, "dp", None)
    own = P("rep", "dp", None)
    return jax.shard_map(
        step,
        mesh=mesh,
        in_specs=(both, both, rows, rows, rows),
        out_specs=(both, own, own, own),
        check_vma=False,
    )
```

```python
import functools

import jax
import jax.numpy as jnp
from jax import lax
from jax.experimental import pallas as pl
from jax.experimental.pallas import tpu as pltpu
from jax.sharding import PartitionSpec as P

MESH = pl.DeviceIdType.MESH
BF16, F32 = jnp.bfloat16, jnp.float32
LAYERS, T, D, FF = 2, 1024, 896, 4736
N = 16
TILE = 256
TILES = 19
FFP = TILE * TILES
RG, RD = D // N, FF // N
EPS = 1e-6
CH = 128
ROW_CHUNKS = 2
ROWS = T // ROW_CHUNKS

DOWN = 2
COLUMNS = {0: (0, 12), 1: (12, TILES)}
GU_A = {0: 8 * 128, 1: 4 * 128}
UNIT_KINDS = (0, 1, DOWN, 0, 1, DOWN)
UNITS, HOPS, ITEMS = len(UNIT_KINDS), 7, 2
LAYER_1 = 3
D_A = 96
D_B = RD - 2 * D_A
STAGGER = 4
PER_UNIT = STAGGER * 2 * ITEMS
READY = 2 * PER_UNIT + 1
N_PIECES = ((0, 512), (512, 384))


class Place:
    def __init__(self):
        self.rep = lax.axis_index("rep")
        me = lax.axis_index("dp")
        self.core = lax.rem(me, 2)
        self.chip = me // 2
        self.ring = jnp.where(self.chip < 4, self.chip, 11 - self.chip)
        self.way = 1 - 2 * self.core
        self.next = (self.rep, self.device(1))
        self.prev = (self.rep, self.device(-1))
        self.sibling = (self.rep, self.chip * 2 + 1 - self.core)
        self.other = (1 - self.rep, me)

    def chip_at(self, steps):
        r = lax.rem(self.ring + self.way * steps + 16, 8)
        return jnp.where(r < 4, r, 11 - r)

    def device(self, steps):
        return self.chip_at(steps) * 2 + self.core


def barrier(devices):
    sem = pltpu.get_barrier_semaphore()
    for device in devices:
        pl.semaphore_signal(sem, inc=1, device_id=device, device_id_type=MESH)
    pl.semaphore_wait(sem, len(devices))


def remote(src, dst, send, recv, device):
    return pltpu.make_async_remote_copy(
        src_ref=src, dst_ref=dst, send_sem=send, recv_sem=recv, device_id=device, device_id_type=MESH
    )


def loop(lo, hi, body):
    def run(i, carry):
        body(i)
        return carry

    lax.fori_loop(lo, hi, run, 0)


def start(copies):
    for copy in copies:
        copy.start()


def wait(copies):
    for copy in copies:
        copy.wait()


def mult(x, m):
    return pl.multiple_of(x, m)


def dot(a, b, dims=((1,), (0,))):
    return lax.dot_general(a, b, (dims, ((), ())), preferred_element_type=F32)


class Gather:
    def __init__(self, here, sources, g_out, d_out, sems):
        self.here, self.sources, self.g_out, self.d_out = here, sources, g_out, d_out
        self.ring_recv, self.x_recv, self.sib_recv, self.ring_send, self.x_send, self.sib_send = sems

    @staticmethod
    def columns(kind):
        first, end = COLUMNS[kind]
        return first * TILE, min(end * TILE, FF) - first * TILE

    def cut(self, kind, is_own, group):
        if kind == DOWN:
            return (pl.ds(mult(D_B + D_A * group, 8), D_A) if is_own else pl.ds(0, D_B)), pl.ds(0, D)
        first, size = self.columns(kind)
        common = size - 2 * GU_A[kind]
        if is_own:
            return pl.ds(0, RG), pl.ds(mult(first + common + GU_A[kind] * group, 128), GU_A[kind])
        return pl.ds(0, RG), pl.ds(first, common)

    def region(self, l, kind, dev, is_own, group):
        rows, cols = self.cut(kind, is_own, group)
        if kind == DOWN:
            return self.d_out.at[l, pl.ds(mult(dev * RD + rows.start, 8), rows.size), cols]
        return self.g_out.at[l, :, pl.ds(mult(dev * RG, 8), RG), cols]

    def send_ring(self, src, dst, u, t, item):
        return remote(src, dst, self.ring_send.at[u], self.ring_recv.at[u, t - 1, item], self.here.next)

    def send_x(self, reg, u, t):
        return remote(reg, reg, self.x_send.at[u], self.x_recv.at[u, t - 1], self.here.other)

    def send_sibling(self, src, dst, u):
        return remote(src, dst, self.sib_send.at[u], self.sib_recv.at[u], self.here.sibling)

    def start_own(self, u, l, kind):
        me = self.here.device(0)
        sources = [ref.at[l] for ref in (self.sources[2:] if kind == DOWN else self.sources[:2])]
        for item in range(ITEMS):
            rows, cols = self.cut(kind, item == 0, self.here.rep)
            to = self.region(l, kind, me, item == 0, self.here.rep)
            for m, src in enumerate(sources):
                self.send_ring(src.at[rows, cols], to if kind == DOWN else to.at[m], u, 1, item).start()
        for m, src in enumerate(sources):
            if kind == DOWN:
                self.send_sibling(src, self.d_out.at[l, pl.ds(mult(me * RD, 8), RD), :], u).start()
            else:
                cols = pl.ds(*self.columns(kind))
                to = self.g_out.at[l, m, pl.ds(mult(me * RG, 8), RG), cols]
                self.send_sibling(src.at[:, cols], to, u).start()

    def ring_event(self, u, l, kind, t, item):
        is_own = item == 0
        reg = self.region(l, kind, self.here.device(-t), is_own, self.here.rep)
        self.send_ring(reg, reg, u, t, item).wait_recv()
        pl.when(t < HOPS)(lambda: self.send_ring(reg, reg, u, t + 1, item).start())
        if is_own:
            self.send_x(reg, u, t).start()
        self.send_sibling(reg, reg, u).start()

    def x_event(self, u, l, kind, t):
        reg = self.region(l, kind, self.here.device(-t), True, 1 - self.here.rep)
        self.send_x(reg, u, t).wait_recv()
        self.send_sibling(reg, reg, u).start()

    def event(self, e):
        round_, place = e // (2 * ITEMS), lax.rem(e, 2 * ITEMS)
        newer, item = place // ITEMS, lax.rem(place, ITEMS)

        def at(round_):
            return (round_ + STAGGER) // STAGGER - 2 + newer, lax.rem(round_, STAGGER) + STAGGER * (1 - newer)

        def of_kind(u, kind):
            first, *others = [i for i in range(UNITS) if UNIT_KINDS[i] == kind]
            return functools.reduce(lambda so_far, i: so_far | (u == i), others, u == first)

        u, t = at(round_)
        l = jnp.where(u < LAYER_1, 0, 1)
        was, hop = at(round_ - 1)
        was_l = jnp.where(was < LAYER_1, 0, 1)
        crosses = (item == 0) & (hop > 0) & (round_ > 0)
        for kind in sorted(set(UNIT_KINDS)):

            @pl.when(of_kind(u, kind))
            def _(kind=kind):
                pl.when((t == 0) & (item == 0))(functools.partial(self.start_own, u, l, kind))
                for i in range(ITEMS):
                    pl.when((t > 0) & (item == i))(functools.partial(self.ring_event, u, l, kind, t, i))

            pl.when(crosses & of_kind(was, kind))(functools.partial(self.x_event, was, was_l, kind, hop))

    def events(self, lo, hi):
        loop(lo, hi, self.event)

    def whole(self, l, kind, of_gu, of_d):
        if kind == DOWN:
            return self.d_out.at[l, pl.ds(0, of_d), :]
        rows, width = of_gu
        return self.g_out.at[l, :, pl.ds(0, rows), pl.ds(0, width)]

    def wait_unit(self, u):
        kind, l = UNIT_KINDS[u], int(u >= LAYER_1)
        width = 0 if kind == DOWN else self.columns(kind)[1]
        half = self.whole(l, kind, (D // 2, width), FF // 2)
        self.send_sibling(half, half, u).wait_recv()

    def wait_sends(self, u):
        kind, l = UNIT_KINDS[u], int(u >= LAYER_1)
        width, own = (0, 0) if kind == DOWN else (self.columns(kind)[1], GU_A[kind])
        sent = (
            self.whole(l, kind, (HOPS * RG, width - own), HOPS * (D_A + D_B)),
            self.whole(l, kind, (HOPS * RG, own), HOPS * D_A),
            self.whole(l, kind, (D // 2, width), FF // 2),
        )
        for ref, sem in zip(sent, (self.ring_send, self.x_send, self.sib_send)):
            remote(ref, ref, sem.at[u], sem.at[u], self.here.next).wait_send()


def along(k, points):
    out = points[-1][1]
    for (k0, e0), (k1, e1) in reversed(list(zip(points, points[1:]))):
        out = jnp.where(k < k1, e0 + (k - k0) * (e1 - e0) // (k1 - k0), out)
    return out


TILE_POINTS = (
    ((0, 0), (24, PER_UNIT), (2 * TILES, 2 * PER_UNIT)),
    ((0, 3 * PER_UNIT), (24, 4 * PER_UNIT), (2 * TILES, 4 * PER_UNIT + 10)),
)
FORWARD_END = READY + TILE_POINTS[1][-1][1]
GATHER_END = READY + (UNITS - 1) * PER_UNIT


def forward_pass(
    here, gather, x_ref, g_out, d_out, p_out, q_out, actt_out, at_out, h1_out, local_sem, w_sem, o_sem, wd_sem, at_sem,
    a_s, h_s, at_s, prod_s, wd_s, wgu_t, both_s, p_s, q_s, pt_s, zc, zr,
):
    load_x = pltpu.make_async_copy(x_ref, h_s, at_sem.at[0])
    load_x.start()
    gather.events(ITEMS, 2 * ITEMS)
    zc[...] = jnp.zeros_like(zc)
    zr[...] = jnp.zeros_like(zr)
    both_s[...] = jnp.zeros_like(both_s)
    me = here.device(0)
    wg_ref, wu_ref, wd_ref = gather.sources
    locals_ = []
    for l in range(LAYERS):
        for m in range(2):
            locals_.append((zc, g_out.at[l, m, :, pl.ds(FF, FFP - FF)]))
            locals_.append(((wg_ref, wu_ref)[m].at[l], g_out.at[l, m, pl.ds(mult(me * RG, 8), RG), pl.ds(0, FF)]))
        locals_.append((zr, d_out.at[l, pl.ds(FF, FFP - FF), :]))
        locals_.append((wd_ref.at[l], d_out.at[l, pl.ds(mult(me * RD, 8), RD), :]))
    locals_ = [pltpu.make_async_copy(src, dst, local_sem.at[i]) for i, (src, dst) in enumerate(locals_)]
    start(locals_)
    load_x.wait()

    def put_at(l):
        return pltpu.make_async_copy(at_s, at_out.at[l], at_sem.at[0])

    put_h = pltpu.make_async_copy(h_s, h1_out, at_sem.at[1])

    def norm(l, first_event, count):
        def chunk(i):
            rows = pl.ds(mult(i * CH, CH), CH)
            wide = h_s[rows, :].astype(F32)
            a = (wide * lax.rsqrt(jnp.mean(wide * wide, -1, keepdims=True) + EPS)).astype(BF16)
            a_s[rows, :] = a
            at_s[:, rows] = a.T
            gather.events(first_event + i * count, first_event + (i + 1) * count)

        loop(0, T // CH, chunk)
        put_at(l).start()

    def add_mlp(first_event):
        parts = [
            pltpu.make_async_copy(d_out.at[0, :, pl.ds(*piece)], wd_s.at[:, pl.ds(*piece)], wd_sem.at[i])
            for i, piece in enumerate(N_PIECES)
        ]
        start(parts)
        for i, piece in enumerate(N_PIECES):
            parts[i].wait()
            cols = pl.ds(*piece)

            def rows_part(r):
                rows = pl.ds(mult(r * ROWS, ROWS), ROWS)
                y = dot(prod_s[rows, :], wd_s[:, cols]).astype(BF16).astype(F32)
                h_s[rows, cols] = (h_s[rows, cols].astype(F32) + y).astype(BF16)
                now = first_event + (i * ROW_CHUNKS + r) * ITEMS
                gather.events(now, now + ITEMS)

            loop(0, ROW_CHUNKS, rows_part)

    def layer(l):
        def loads(j, slot):
            cols = pl.ds(mult(j * TILE, TILE), TILE)
            return [
                pltpu.make_async_copy(
                    g_out.at[l, m, :, cols], wgu_t.at[slot, :, pl.ds(m * TILE, TILE)], w_sem.at[slot, m]
                )
                for m in range(2)
            ]

        def stores(j, slot):
            rows = pl.ds(mult(j * TILE, TILE), TILE)
            pairs = ((p_s, p_out.at[l, j]), (q_s, q_out.at[l, j]), (pt_s, actt_out.at[l, rows, :]))
            return [pltpu.make_async_copy(src.at[slot], dst, o_sem.at[slot, i]) for i, (src, dst) in enumerate(pairs)]

        def done_by(k):
            return READY + jnp.where(l == 0, along(k, TILE_POINTS[0]), along(k, TILE_POINTS[1]))

        firsts = {u: COLUMNS[kind][0] for u, kind in enumerate(UNIT_KINDS) if kind != DOWN}

        def tick(j):
            slot = lax.rem(j, 2)
            for u, first in firsts.items():

                @pl.when((j == first) & ((l == 0) == (u < LAYER_1)))
                def _(u=u):
                    gather.wait_unit(u)

            is_first, next_is_first = ((k == 0) | (k == COLUMNS[1][0]) for k in (j, j + 1))
            pl.when(is_first)(lambda: start(loads(j, slot)))
            pl.when((j + 1 < TILES) & ~next_is_first)(lambda: start(loads(j + 1, 1 - slot)))
            wait(loads(j, slot))
            before = jnp.maximum(j - 1, 0)
            for r in range(ROW_CHUNKS):
                hidden(1 - r, j if r else before, slot if r else 1 - slot)
                both_s[r] = dot(a_s[pl.ds(r * ROWS, ROWS), :], wgu_t[slot])
                if r == 0:
                    pl.when(j >= 1)(lambda: start(stores(j - 1, 1 - slot)))
                    pl.when(j >= 2)(lambda: wait(stores(j - 2, slot)))
                gather.events(done_by(2 * j + r), done_by(2 * j + r + 1))

        def hidden(r, j, slot):
            rows = pl.ds(r * ROWS, ROWS)
            gate, up = both_s[r, :, pl.ds(0, TILE)], both_s[r, :, pl.ds(TILE, TILE)]
            s = 0.5 * jnp.tanh(0.5 * gate) + 0.5
            q = gate * s
            q_s[slot, rows, :] = q
            p_s[slot, rows, :] = up * (s + q * (1 - s))
            prod = (q * up).astype(BF16)
            pt_s[slot, :, rows] = prod.T
            prod_s[rows, pl.ds(mult(j * TILE, TILE), TILE)] = prod

        loop(0, TILES, tick)
        last = TILES - 1
        hidden(1, last, last % 2)
        start(stores(last, last % 2))
        for j in (last - 1, last):
            wait(stores(j, j % 2))

        @pl.when(l == 0)
        def _():
            gather.wait_unit(UNIT_KINDS.index(DOWN))
            now = READY + 2 * PER_UNIT
            put_at(0).wait()
            add_mlp(now)
            now += ITEMS * ROW_CHUNKS * len(N_PIECES)
            norm(1, now, 1)
            put_h.start()

    norm(0, 2 * ITEMS, 1)
    gather.events(2 * ITEMS + T // CH, READY)
    wait(locals_)
    loop(0, LAYERS, layer)
    put_h.wait()
    put_at(1).wait()


PAIRS, STEPS, PLACES = 4, 8, 4
PER_PAIR = STEPS // 2 * PLACES
QUEUE = LAYERS * PAIRS + 1
SECOND = PAIRS + 1
D_PARTS = ((0, 152), (152, 144))
BIG = 2 * TILE
BIGS = (TILES + 1) // 2
PART_BIGS = 3
C_PART = PART_BIGS * BIG
C_LAST = FF - 2 * C_PART
D_PIECE, C_PIECE = 72, 6 * 128
LAST_EVENT = (QUEUE + 1) * PER_PAIR
AHEAD = PLACES - 1
LAG = 2 * PLACES
BEFORE, BETWEEN, AFTER = (2, 63), (12, 74), (63, 120)


def backward_pass(
    here, gather, dy_ref, x_ref, h1_ref, g_ref, d_ref, p_ref, q_ref, actt_ref, at_ref,
    dx_out, dg_out, du_out, dd_out, own_gu, sib_gu, own_d, sib_d, slot_d, slot_c,
    red_recv, red_send, st_sem, fin_sem, sd_recv, sgu_recv, lhs_sem, blk_sem, blk_send, w_sem, term_sem, term_send, misc_sem,
    dh_s, at_s, h_s, dacc, lhs_t, blk_s, wgu_t, wd_t, p_t, q_t, dz_s, term_s, st_d, st_c,
):
    def chips(s):
        return here.chip_at(-1 - s), here.chip_at(1 + s)

    class Lane:
        def __init__(self, l, pair, lane, s, place, down, last):
            chip, _ = chips(s)
            self.s, self.place, self.lane = s, place, lane
            self.sems = [sem.at[l, pair, lane] for sem in (red_recv, red_send)]
            self.fin = fin_sem.at[l, pair, lane]
            if down:
                first, size = D_PARTS[last]
                rows, cut = pl.ds(first, size), pl.ds(0, size)
                pieces = [pl.ds(0, D_PIECE), pl.ds(D_PIECE, size - D_PIECE)]
                self.slot = slot_d.at[lane, s, cut, :]
                self.slots = [[slot_d.at[lane, to, piece, :] for to in (s, s + 1)] for piece in pieces]
                self.ends = [[st_d.at[place, i, piece, :] for i in range(2)] for piece in pieces]
                self.st = [st_d.at[place, i, cut, :] for i in range(2)]
                self.terms = [ref.at[l, chip, rows, :] for ref in (own_d, sib_d)]
                self.result = dd_out.at[l, rows, :]
            else:
                part = pair - 1
                size = C_LAST if last else C_PART
                cols, cut = (pl.ds(first, size) for first in (mult(part * C_PART, 128), 0))
                pieces = [pl.ds(0, C_PIECE), pl.ds(C_PIECE, size - C_PIECE)]
                self.slot = slot_c.at[part, lane, s, :, cut]
                self.slots = [[slot_c.at[part, lane, to, :, piece] for to in (s, s + 1)] for piece in pieces]
                self.ends = [[st_c.at[place, i, :, piece] for i in range(2)] for piece in pieces]
                self.st = [st_c.at[place, i, :, cut] for i in range(2)]
                self.terms = [ref.at[l, lane, chip, :, cols] for ref in (own_gu, sib_gu)]
                self.result = [out.at[l, :, cols] for out in (dg_out, du_out)]

        def stage(self):
            pairs = zip(self.terms, self.st)
            return [pltpu.make_async_copy(a, b, st_sem.at[self.place, i]) for i, (a, b) in enumerate(pairs)]

        def send(self, to, piece):
            recv, sent = self.sems
            src, dst = self.slots[piece][0], self.slots[piece][to]
            return remote(src, dst, sent.at[self.s, piece], recv.at[self.s + to, piece], here.next)

        def finish(self, action):
            if not isinstance(self.result, list):
                action(pltpu.make_async_copy(self.slot, self.result, self.fin))
                return
            for lane, result in enumerate(self.result):
                copy = pltpu.make_async_copy(self.slot, result, self.fin)
                pl.when(self.lane == lane)(functools.partial(action, copy))

        def step(self):
            wait(self.stage())
            for i in range(2):
                slot = self.slots[i][0]
                own, sib = (end[...].astype(F32) for end in self.ends[i])
                total = own + sib

                @pl.when(self.s > 0)
                def _():
                    self.send(0, i).wait_recv()
                    slot[...] = (slot[...].astype(F32) + total).astype(BF16)

                @pl.when(self.s == 0)
                def _():
                    slot[...] = total.astype(BF16)

                pl.when(self.s < STEPS - 1)(lambda: self.send(1, i).start())
            pl.when(self.s == STEPS - 1)(lambda: self.finish(lambda copy: copy.start()))

        def wait_out(self):
            for i in range(2):
                pl.when(self.s < STEPS - 1)(lambda: self.send(1, i).wait_send())
            pl.when(self.s == STEPS - 1)(lambda: self.finish(lambda copy: copy.wait()))

        def prefetch(self):
            start(self.stage())

    def with_lane(e, action, ahead_of=lambda l, pair, lane, s: None):
        round_, place = e // PLACES, lax.rem(e, PLACES)
        new = place // 2
        index = round_ // PLACES + new - 1
        s = lax.rem(round_, PLACES) + PLACES * (1 - new)
        lane = lax.rem(place, 2)

        @pl.when((index >= 0) & (index < QUEUE) & (index != 1))
        def _():
            second = jnp.where(index < SECOND, 0, 1)
            free = jnp.where((index > 1) & (index < SECOND), 1, 0)
            l, pair = 1 - second, index - SECOND * second - free
            ahead_of(l, pair, lane, s)
            for is_down, is_last, chosen in (
                (True, False, (pair == 0) & (lane == 0)), (True, True, (pair == 0) & (lane == 1)),
                (False, False, (pair > 0) & (pair < PAIRS - 1)), (False, True, pair == PAIRS - 1),
            ):
                pl.when(chosen)(lambda: action(Lane(l, pair, lane, s, place, is_down, is_last)))

    def terms_ready(l, pair, lane, s):
        @pl.when((pair == 0) & (lane == 0))
        def _():
            whole = sib_d.at[l, 0]
            remote(whole, whole, blk_send.at[0], sd_recv.at[l, s], here.sibling).wait_recv()

        @pl.when((pair > 0) & (lane == 0) & (s == 0))
        def _():
            for is_last in (False, True):
                width = FFP - 2 * C_PART if is_last else C_PART

                @pl.when((pair == PAIRS - 1) == is_last)
                def _(width=width):
                    part = sib_gu.at[l, :, :, :, pl.ds(0, width)]
                    sem = sgu_recv.at[l, pair - 1]
                    remote(part, part, term_send.at[0, 0], sem, here.sibling).wait_recv()

    def events(lo, hi):
        loop(lo, hi, event)

    def fetch(e):
        with_lane(e, Lane.prefetch, terms_ready)

    def event(e):
        pl.when(e >= LAG)(lambda: with_lane(e - LAG, Lane.wait_out))
        fetch(e + AHEAD)
        with_lane(e, Lane.step)

    def lhs_loads(l, s, slot):
        mine, other = chips(s)
        rows = ((mine * 2 + here.core) * RD, (other * 2 + 1 - here.core) * RD)
        return [
            pltpu.make_async_copy(actt_ref.at[l, pl.ds(mult(row, 8), RD), :], lhs_t.at[slot, i], lhs_sem.at[slot, i])
            for i, row in enumerate(rows)
        ]

    def block_copies(l, s, slot):
        mine, other = chips(s)
        return (
            pltpu.make_async_copy(blk_s.at[slot, 0], own_d.at[l, mine], blk_sem.at[slot]),
            remote(blk_s.at[slot, 1], sib_d.at[l, other], blk_send.at[slot], sd_recv.at[l, s], here.sibling),
        )

    def both_halves(j, action):
        action(0)
        pl.when(j < BIGS - 1)(lambda: action(1))

    def tile_loads(l, j, slot, half):
        tile = 2 * j + half
        src = pl.ds(mult(tile * TILE, TILE), TILE)
        dst = pl.ds(half * TILE, TILE)
        pairs = [
            (d_ref.at[l, src, :], wd_t.at[slot, dst, :]),
            (p_ref.at[l, tile], p_t.at[slot, :, dst]),
            (q_ref.at[l, tile], q_t.at[slot, :, dst]),
        ]
        pairs += [(g_ref.at[l, m, :, src], wgu_t.at[slot, :, pl.ds((2 * half + m) * TILE, TILE)]) for m in range(2)]
        return [pltpu.make_async_copy(src, dst, w_sem.at[slot, half, i]) for i, (src, dst) in enumerate(pairs)]

    def term_copies(l, j, half):
        cols = pl.ds(mult((2 * j + half) * TILE, TILE), TILE)
        part = jnp.minimum(j // PART_BIGS, PAIRS - 2)
        own, sib = [], []
        for m in range(2):
            mine, other = term_s.at[half, m, :, here.core], term_s.at[half, m, :, 1 - here.core]
            own.append(pltpu.make_async_copy(mine, own_gu.at[l, m, :, :, cols], term_sem.at[half, m]))
            to = sib_gu.at[l, m, :, :, cols]
            sib.append(remote(other, to, term_send.at[half, m], sgu_recv.at[l, part], here.sibling))
        return own, sib

    def start_terms(l, j, half):
        own, sib = term_copies(l, j, half)
        start(own + sib)

    def wait_terms(l, j, half):
        own, sib = term_copies(l, j, half)
        wait(own)
        for copy in sib:
            copy.wait_send()

    def wait_block(l, s, slot):
        own, sib = block_copies(l, s, slot)
        own.wait()
        sib.wait_send()

    def layer(i):
        l = 1 - i
        before, between, after = (jnp.where(i == 0, *counts) for counts in (BEFORE, BETWEEN, AFTER))
        load_at = pltpu.make_async_copy(at_ref.at[l], at_s, misc_sem.at[0])
        load_at.start()
        pl.when(i == 0)(pltpu.make_async_copy(h1_ref, h_s, misc_sem.at[1]).start)
        pl.when(i == 1)(pltpu.make_async_copy(x_ref, h_s, misc_sem.at[1]).start)
        for s in range(2):
            start(lhs_loads(l, s, s))
        first_loads = lambda: both_halves(0, lambda half: start(tile_loads(l, 0, 0, half)))
        pl.when(i == 1)(first_loads)

        def pair(s):
            slot = lax.rem(s, 2)
            there = lax.rem(s, 3)
            pl.when(s < STEPS - 2)(lambda: start(lhs_loads(l, s + 2, lax.rem(s + 2, 3))))
            wait(lhs_loads(l, s, there))
            for b in range(2):
                blk_s[slot, b] = dot(lhs_t[there, b], dh_s[...]).astype(BF16)
            start(block_copies(l, s, slot))

            @pl.when(i == 0)
            def _():
                lo, hi = (FORWARD_END + (GATHER_END - FORWARD_END) * to // STEPS for to in (s, s + 1))
                gather.events(lo, hi)

            pl.when(s >= 1)(lambda: wait_block(l, s - 1, 1 - slot))
            pl.when((i == 0) & (s == 1))(lambda: loop(BEFORE[0], BEFORE[0] + AHEAD, fetch))

            def done_by(s):
                cap = jnp.where(i == 0, jnp.maximum(PLACES * s - 1, before), LAST_EVENT)
                return jnp.minimum(before + ((between - before) * (s + 1)) // STEPS, cap)

            loop(jnp.where(s == 0, before, done_by(s - 1)), done_by(s), event)

        loop(0, STEPS, pair)
        wait_block(l, STEPS - 1, (STEPS - 1) % 2)

        @pl.when(i == 0)
        def _():
            gather.wait_unit(UNITS - 1)
            first_loads()

        load_at.wait()
        dacc[...] = jnp.zeros_like(dacc)

        def tick(j):
            slot = lax.rem(j, 2)
            pl.when(j + 1 < BIGS)(lambda: both_halves(j + 1, lambda half: start(tile_loads(l, j + 1, 1 - slot, half))))
            both_halves(j, lambda half: wait(tile_loads(l, j, slot, half)))

            @pl.when(j == BIGS - 1)
            def _():
                for ref in (p_t, q_t):
                    ref[slot, :, pl.ds(TILE, TILE)] = jnp.zeros((T, TILE), F32)

            def done_by(k):
                ready = jnp.maximum(k - 2, 0) // (PART_BIGS * 4)
                cap = jnp.where(i == 0, PER_PAIR * (2 + jnp.minimum(ready, PAIRS - 2)) - 1, LAST_EVENT)
                return jnp.minimum(between + (k * (after - between)) // (4 * BIGS), cap)

            def quarter(k):
                events(done_by(4 * j + k), done_by(4 * j + k + 1))

            for r in range(2):
                rows = pl.ds(r * ROWS, ROWS)
                dprod = dot(dh_s[rows, :], wd_t[slot], ((1,), (1,))).astype(BF16).astype(F32)
                by_gate = (dprod * p_t[slot, rows, :]).astype(BF16)
                by_up = (dprod * q_t[slot, rows, :]).astype(BF16)
                for half in range(2):
                    for m, by in enumerate((by_gate, by_up)):
                        part = by[:, half * TILE : (half + 1) * TILE]
                        dz_s[rows, pl.ds((2 * half + m) * TILE, TILE)] = part
                dacc[rows, :] += dot(dz_s[rows, :], wgu_t[slot], ((1,), (1,)))
                if r == 1:
                    pl.when(j > 0)(lambda: [wait_terms(l, j - 1, half) for half in range(2)] and None)
                quarter(r)
            for r in range(2):
                term = dot(at_s[pl.ds(r * D // 2, D // 2), :], dz_s[...])
                for b in range(8):
                    for half in range(2):
                        for m in range(2):
                            col = (2 * half + m) * TILE
                            block = term[b * RG : (b + 1) * RG, col : col + TILE]
                            term_s[half, m, r * 4 + b // 2, b % 2] = block.astype(BF16)
                if r == 1:
                    both_halves(j, lambda half: start_terms(l, j, half))
                quarter(2 + r)

        loop(0, BIGS, tick)
        wait_terms(l, BIGS - 1, 0)
        pltpu.make_async_copy(h1_ref, h_s, misc_sem.at[1]).wait()

        def new_dh(r):
            rows = pl.ds(mult(r * CH, CH), CH)
            da = dacc[rows, :].astype(BF16).astype(F32)
            wide = h_s[rows, :].astype(F32)
            scale = lax.rsqrt(jnp.mean(wide * wide, -1, keepdims=True) + EPS)
            along = jnp.mean(da * wide, -1, keepdims=True) * scale * scale
            by_h = (scale * (da - wide * along)).astype(BF16).astype(F32)
            dh_s[rows, :] = (dh_s[rows, :].astype(F32) + by_h).astype(BF16)

        loop(0, T // CH, new_dh)

    load_dy = pltpu.make_async_copy(dy_ref, dh_s, misc_sem.at[2])
    load_dy.start()
    load_dy.wait()
    loop(0, LAYERS, layer)
    put_dx = pltpu.make_async_copy(dh_s, dx_out, misc_sem.at[2])
    put_dx.start()
    loop(AFTER[1], LAST_EVENT, event)
    loop(LAST_EVENT - LAG, LAST_EVENT, lambda e: with_lane(e, Lane.wait_out))
    put_dx.wait()


def kernel(
    dy_ref, x_ref, wg_ref, wu_ref, wd_ref,
    dx_out, dg_out, du_out, dd_out, own_gu, sib_gu, own_d, sib_d, g_out, d_out, p_out, q_out, actt_out, at_out, h1_out,
    slot_d, slot_c, *sems,
):
    gather_sems, forward_sems, backward_sems = sems[:6], sems[6:11], sems[11:]
    here = Place()
    barrier((here.next, here.prev, here.sibling, here.other))
    gather = Gather(here, (wg_ref, wu_ref, wd_ref), g_out, d_out, gather_sems)
    vmem = pltpu.VMEM
    two = (2, 2)
    pl.run_scoped(
        functools.partial(
            forward_pass, here, gather, x_ref, g_out, d_out, p_out, q_out, actt_out, at_out, h1_out, *forward_sems
        ),
        vmem((T, D), BF16),
        vmem((T, D), BF16),
        vmem((D, T), BF16),
        vmem((T, FFP), BF16),
        vmem((FFP, D), BF16),
        vmem((2, D, 2 * TILE), BF16),
        vmem((2, ROWS, 2 * TILE), F32),
        vmem((2, T, TILE), F32),
        vmem((2, T, TILE), F32),
        vmem((2, TILE, T), BF16),
        vmem((D, FFP - FF), BF16),
        vmem((FFP - FF, D), BF16),
    )
    pl.run_scoped(
        functools.partial(
            backward_pass, here, gather, dy_ref, x_ref, h1_out, g_out, d_out, p_out, q_out, actt_out, at_out,
            dx_out, dg_out, du_out, dd_out, own_gu, sib_gu, own_d, sib_d, slot_d, slot_c, *backward_sems,
        ),
        vmem((T, D), BF16),
        vmem((D, T), BF16),
        vmem((T, D), BF16),
        vmem((T, D), F32),
        vmem((3, 2, RD, T), BF16),
        vmem((*two, RD, D), BF16),
        vmem((2, D, 2 * BIG), BF16),
        vmem((2, BIG, D), BF16),
        vmem((2, T, BIG), F32),
        vmem((2, T, BIG), F32),
        vmem((T, 2 * BIG), BF16),
        vmem((*two, 8, 2, RG, TILE), BF16),
        vmem((PLACES, 2, D_PARTS[0][1], D), BF16),
        vmem((PLACES, 2, RG, C_LAST), BF16),
    )
    for u in range(UNITS):
        gather.wait_sends(u)


def both_passes(dy, x, wg, wu, wd):
    any_, vmem = pl.BlockSpec(memory_space=pl.ANY), pl.BlockSpec(memory_space=pltpu.VMEM)
    dma = pltpu.SemaphoreType.DMA
    shape = jax.ShapeDtypeStruct
    two = (2, 2)
    per_part = (LAYERS, PAIRS, 2)
    outs = (
        shape((T, D), BF16),
        *[shape((LAYERS, RG, FF), BF16)] * 2,
        shape((LAYERS, RD, D), BF16),
        *[shape((LAYERS, 2, 8, RG, FFP), BF16)] * 2,
        *[shape((LAYERS, 8, RD, D), BF16)] * 2,
        shape((LAYERS, 2, D, FFP), BF16),
        shape((LAYERS, FFP, D), BF16),
        *[shape((LAYERS, TILES, T, TILE), F32)] * 2,
        shape((LAYERS, FFP, T), BF16),
        shape((LAYERS, D, T), BF16),
        shape((T, D), BF16),
    )
    gather_sems = [dma((UNITS, HOPS, ITEMS)), dma((UNITS, HOPS)), *[dma((UNITS,))] * 4]
    forward_sems = [dma((LAYERS * 6,)), dma(two), dma((2, 3)), dma((2,)), dma((2,))]
    backward_sems = [
        *[dma((*per_part, STEPS, 2))] * 2,
        dma((PLACES, 2)),
        dma(per_part),
        dma((LAYERS, STEPS)),
        dma((LAYERS, PAIRS - 1)),
        dma((3, 2)),
        dma((2,)),
        dma((2,)),
        dma((*two, 5)),
        dma(two),
        dma(two),
        dma((3,)),
    ]
    return pl.pallas_call(
        kernel,
        out_shape=outs,
        in_specs=[any_] * 2 + [vmem] * 3,
        out_specs=(any_,) * len(outs),
        scratch_shapes=[
            pltpu.VMEM((2, STEPS, D_PARTS[0][1], D), BF16),
            pltpu.VMEM((PAIRS - 1, 2, STEPS, RG, C_LAST), BF16),
            *gather_sems,
            *forward_sems,
            *backward_sems,
        ],
        compiler_params=pltpu.CompilerParams(
            collective_id=0, has_side_effects=True, vmem_limit_bytes=63 * 1024 * 1024
        ),
        name="both_passes",
    )(dy, x, wg, wu, wd)


def solution(mesh):
    def step(x, dy, wg, wu, wd):
        dx, dg, du, dd, *_ = both_passes(dy[0], x[0], wg, wu, wd)
        return dx[None], dg, du, dd

    both, rows = P(("rep", "dp"), None, None), P(None, "dp", None)
    own = P("rep", "dp", None)
    return jax.shard_map(
        step,
        mesh=mesh,
        in_specs=(both, both, rows, rows, rows),
        out_specs=(both, own, own, own),
        check_vma=False,
    )
```

```python
import functools

import jax
import jax.numpy as jnp
from jax import lax
from jax.experimental import pallas as pl
from jax.experimental.pallas import tpu as pltpu
from jax.sharding import PartitionSpec as P

MESH = pl.DeviceIdType.MESH
BF16, F32 = jnp.bfloat16, jnp.float32
LAYERS, T, D, FF = 2, 1024, 896, 4736
N = 16
TILE = 256
TILES = 19
FFP = TILE * TILES
RG, RD = D // N, FF // N
EPS = 1e-6
CH = 128
ROW_CHUNKS = 2
ROWS = T // ROW_CHUNKS

DOWN = 2
COLUMNS = {0: (0, 12), 1: (12, TILES)}
GU_A = {0: 8 * 128, 1: 4 * 128}
UNIT_KINDS = (0, 1, DOWN, 0, 1, DOWN)
UNITS, HOPS, ITEMS = len(UNIT_KINDS), 7, 2
LAYER_1 = 3
D_A = 96
D_B = RD - 2 * D_A
STAGGER = 4
PER_UNIT = STAGGER * 2 * ITEMS
READY = 2 * PER_UNIT + 1
N_PIECES = ((0, 512), (512, 384))


class Place:
    def __init__(self):
        self.rep = lax.axis_index("rep")
        me = lax.axis_index("dp")
        self.core = lax.rem(me, 2)
        self.chip = me // 2
        self.ring = jnp.where(self.chip < 4, self.chip, 11 - self.chip)
        self.way = 1 - 2 * self.core
        self.next = (self.rep, self.device(1))
        self.prev = (self.rep, self.device(-1))
        self.sibling = (self.rep, self.chip * 2 + 1 - self.core)
        self.other = (1 - self.rep, me)

    def chip_at(self, steps):
        r = lax.rem(self.ring + self.way * steps + 16, 8)
        return jnp.where(r < 4, r, 11 - r)

    def device(self, steps):
        return self.chip_at(steps) * 2 + self.core


def barrier(devices):
    sem = pltpu.get_barrier_semaphore()
    for device in devices:
        pl.semaphore_signal(sem, inc=1, device_id=device, device_id_type=MESH)
    pl.semaphore_wait(sem, len(devices))


def remote(src, dst, send, recv, device):
    return pltpu.make_async_remote_copy(
        src_ref=src, dst_ref=dst, send_sem=send, recv_sem=recv, device_id=device, device_id_type=MESH
    )


def loop(lo, hi, body):
    def run(i, carry):
        body(i)
        return carry

    lax.fori_loop(lo, hi, run, 0)


def start(copies):
    for copy in copies:
        copy.start()


def wait(copies):
    for copy in copies:
        copy.wait()


def mult(x, m):
    return pl.multiple_of(x, m)


def dot(a, b, dims=((1,), (0,))):
    return lax.dot_general(a, b, (dims, ((), ())), preferred_element_type=F32)


class Gather:
    def __init__(self, here, sources, g_out, d_out, sems):
        self.here, self.sources, self.g_out, self.d_out = here, sources, g_out, d_out
        self.ring_recv, self.x_recv, self.sib_recv, self.ring_send, self.x_send, self.sib_send = sems

    @staticmethod
    def columns(kind):
        first, end = COLUMNS[kind]
        return first * TILE, min(end * TILE, FF) - first * TILE

    def cut(self, kind, is_own, group):
        if kind == DOWN:
            return (pl.ds(mult(D_B + D_A * group, 8), D_A) if is_own else pl.ds(0, D_B)), pl.ds(0, D)
        first, size = self.columns(kind)
        common = size - 2 * GU_A[kind]
        if is_own:
            return pl.ds(0, RG), pl.ds(mult(first + common + GU_A[kind] * group, 128), GU_A[kind])
        return pl.ds(0, RG), pl.ds(first, common)

    def region(self, l, kind, dev, is_own, group):
        rows, cols = self.cut(kind, is_own, group)
        if kind == DOWN:
            return self.d_out.at[l, pl.ds(mult(dev * RD + rows.start, 8), rows.size), cols]
        return self.g_out.at[l, :, pl.ds(mult(dev * RG, 8), RG), cols]

    def send_ring(self, src, dst, u, t, item):
        return remote(src, dst, self.ring_send.at[u], self.ring_recv.at[u, t - 1, item], self.here.next)

    def send_x(self, reg, u, t):
        return remote(reg, reg, self.x_send.at[u], self.x_recv.at[u, t - 1], self.here.other)

    def send_sibling(self, src, dst, u):
        return remote(src, dst, self.sib_send.at[u], self.sib_recv.at[u], self.here.sibling)

    def start_own(self, u, l, kind):
        me = self.here.device(0)
        sources = [ref.at[l] for ref in (self.sources[2:] if kind == DOWN else self.sources[:2])]
        for item in range(ITEMS):
            rows, cols = self.cut(kind, item == 0, self.here.rep)
            to = self.region(l, kind, me, item == 0, self.here.rep)
            for m, src in enumerate(sources):
                self.send_ring(src.at[rows, cols], to if kind == DOWN else to.at[m], u, 1, item).start()
        for m, src in enumerate(sources):
            if kind == DOWN:
                self.send_sibling(src, self.d_out.at[l, pl.ds(mult(me * RD, 8), RD), :], u).start()
            else:
                cols = pl.ds(*self.columns(kind))
                to = self.g_out.at[l, m, pl.ds(mult(me * RG, 8), RG), cols]
                self.send_sibling(src.at[:, cols], to, u).start()

    def ring_event(self, u, l, kind, t, item):
        is_own = item == 0
        reg = self.region(l, kind, self.here.device(-t), is_own, self.here.rep)
        self.send_ring(reg, reg, u, t, item).wait_recv()
        pl.when(t < HOPS)(lambda: self.send_ring(reg, reg, u, t + 1, item).start())
        if is_own:
            self.send_x(reg, u, t).start()
        self.send_sibling(reg, reg, u).start()

    def x_event(self, u, l, kind, t):
        reg = self.region(l, kind, self.here.device(-t), True, 1 - self.here.rep)
        self.send_x(reg, u, t).wait_recv()
        self.send_sibling(reg, reg, u).start()

    def event(self, e):
        round_, place = e // (2 * ITEMS), lax.rem(e, 2 * ITEMS)
        newer, item = place // ITEMS, lax.rem(place, ITEMS)

        def at(round_):
            return (round_ + STAGGER) // STAGGER - 2 + newer, lax.rem(round_, STAGGER) + STAGGER * (1 - newer)

        def of_kind(u, kind):
            first, *others = [i for i in range(UNITS) if UNIT_KINDS[i] == kind]
            return functools.reduce(lambda so_far, i: so_far | (u == i), others, u == first)

        u, t = at(round_)
        l = jnp.where(u < LAYER_1, 0, 1)
        was, hop = at(round_ - 1)
        was_l = jnp.where(was < LAYER_1, 0, 1)
        crosses = (item == 0) & (hop > 0) & (round_ > 0)
        for kind in sorted(set(UNIT_KINDS)):

            @pl.when(of_kind(u, kind))
            def _(kind=kind):
                pl.when((t == 0) & (item == 0))(functools.partial(self.start_own, u, l, kind))
                for i in range(ITEMS):
                    pl.when((t > 0) & (item == i))(functools.partial(self.ring_event, u, l, kind, t, i))

            pl.when(crosses & of_kind(was, kind))(functools.partial(self.x_event, was, was_l, kind, hop))

    def events(self, lo, hi):
        loop(lo, hi, self.event)

    def whole(self, l, kind, of_gu, of_d):
        if kind == DOWN:
            return self.d_out.at[l, pl.ds(0, of_d), :]
        rows, width = of_gu
        return self.g_out.at[l, :, pl.ds(0, rows), pl.ds(0, width)]

    def wait_unit(self, u):
        kind, l = UNIT_KINDS[u], int(u >= LAYER_1)
        width = 0 if kind == DOWN else self.columns(kind)[1]
        half = self.whole(l, kind, (D // 2, width), FF // 2)
        self.send_sibling(half, half, u).wait_recv()

    def wait_sends(self, u):
        kind, l = UNIT_KINDS[u], int(u >= LAYER_1)
        width, own = (0, 0) if kind == DOWN else (self.columns(kind)[1], GU_A[kind])
        sent = (
            self.whole(l, kind, (HOPS * RG, width - own), HOPS * (D_A + D_B)),
            self.whole(l, kind, (HOPS * RG, own), HOPS * D_A),
            self.whole(l, kind, (D // 2, width), FF // 2),
        )
        for ref, sem in zip(sent, (self.ring_send, self.x_send, self.sib_send)):
            remote(ref, ref, sem.at[u], sem.at[u], self.here.next).wait_send()


def along(k, points):
    out = points[-1][1]
    for (k0, e0), (k1, e1) in reversed(list(zip(points, points[1:]))):
        out = jnp.where(k < k1, e0 + (k - k0) * (e1 - e0) // (k1 - k0), out)
    return out


TILE_POINTS = (
    ((0, 0), (24, PER_UNIT), (2 * TILES, 2 * PER_UNIT)),
    ((0, 3 * PER_UNIT), (24, 4 * PER_UNIT), (2 * TILES, 4 * PER_UNIT + 10)),
)
FORWARD_END = READY + TILE_POINTS[1][-1][1]
GATHER_END = READY + (UNITS - 1) * PER_UNIT


def forward_pass(
    here, gather, x_ref, g_out, d_out, p_out, q_out, actt_out, at_out, h1_out, local_sem, w_sem, o_sem, wd_sem, at_sem,
    a_s, h_s, at_s, prod_s, wd_s, wgu_t, both_s, p_s, q_s, pt_s, zc, zr,
):
    load_x = pltpu.make_async_copy(x_ref, h_s, at_sem.at[0])
    load_x.start()
    gather.events(ITEMS, 2 * ITEMS)
    zc[...] = jnp.zeros_like(zc)
    zr[...] = jnp.zeros_like(zr)
    both_s[...] = jnp.zeros_like(both_s)
    me = here.device(0)
    wg_ref, wu_ref, wd_ref = gather.sources
    locals_ = []
    for l in range(LAYERS):
        for m in range(2):
            locals_.append((zc, g_out.at[l, m, :, pl.ds(FF, FFP - FF)]))
            locals_.append(((wg_ref, wu_ref)[m].at[l], g_out.at[l, m, pl.ds(mult(me * RG, 8), RG), pl.ds(0, FF)]))
        locals_.append((zr, d_out.at[l, pl.ds(FF, FFP - FF), :]))
        locals_.append((wd_ref.at[l], d_out.at[l, pl.ds(mult(me * RD, 8), RD), :]))
    locals_ = [pltpu.make_async_copy(src, dst, local_sem.at[i]) for i, (src, dst) in enumerate(locals_)]
    start(locals_)
    load_x.wait()

    def put_at(l):
        return pltpu.make_async_copy(at_s, at_out.at[l], at_sem.at[0])

    put_h = pltpu.make_async_copy(h_s, h1_out, at_sem.at[1])

    def norm(l, first_event, count):
        def chunk(i):
            rows = pl.ds(mult(i * CH, CH), CH)
            wide = h_s[rows, :].astype(F32)
            a = (wide * lax.rsqrt(jnp.mean(wide * wide, -1, keepdims=True) + EPS)).astype(BF16)
            a_s[rows, :] = a
            at_s[:, rows] = a.T
            gather.events(first_event + i * count, first_event + (i + 1) * count)

        loop(0, T // CH, chunk)
        put_at(l).start()

    def add_mlp(first_event):
        parts = [
            pltpu.make_async_copy(d_out.at[0, :, pl.ds(*piece)], wd_s.at[:, pl.ds(*piece)], wd_sem.at[i])
            for i, piece in enumerate(N_PIECES)
        ]
        start(parts)
        for i, piece in enumerate(N_PIECES):
            parts[i].wait()
            cols = pl.ds(*piece)

            def rows_part(r):
                rows = pl.ds(mult(r * ROWS, ROWS), ROWS)
                y = dot(prod_s[rows, :], wd_s[:, cols]).astype(BF16).astype(F32)
                h_s[rows, cols] = (h_s[rows, cols].astype(F32) + y).astype(BF16)
                now = first_event + (i * ROW_CHUNKS + r) * ITEMS
                gather.events(now, now + ITEMS)

            loop(0, ROW_CHUNKS, rows_part)

    def layer(l):
        def loads(j, slot):
            cols = pl.ds(mult(j * TILE, TILE), TILE)
            return [
                pltpu.make_async_copy(
                    g_out.at[l, m, :, cols], wgu_t.at[slot, :, pl.ds(m * TILE, TILE)], w_sem.at[slot, m]
                )
                for m in range(2)
            ]

        def stores(j, slot):
            rows = pl.ds(mult(j * TILE, TILE), TILE)
            pairs = ((p_s, p_out.at[l, j]), (q_s, q_out.at[l, j]), (pt_s, actt_out.at[l, rows, :]))
            return [pltpu.make_async_copy(src.at[slot], dst, o_sem.at[slot, i]) for i, (src, dst) in enumerate(pairs)]

        def done_by(k):
            return READY + jnp.where(l == 0, along(k, TILE_POINTS[0]), along(k, TILE_POINTS[1]))

        firsts = {u: COLUMNS[kind][0] for u, kind in enumerate(UNIT_KINDS) if kind != DOWN}

        def tick(j):
            slot = lax.rem(j, 2)
            for u, first in firsts.items():

                @pl.when((j == first) & ((l == 0) == (u < LAYER_1)))
                def _(u=u):
                    gather.wait_unit(u)

            is_first, next_is_first = ((k == 0) | (k == COLUMNS[1][0]) for k in (j, j + 1))
            pl.when(is_first)(lambda: start(loads(j, slot)))
            pl.when((j + 1 < TILES) & ~next_is_first)(lambda: start(loads(j + 1, 1 - slot)))
            wait(loads(j, slot))
            before = jnp.maximum(j - 1, 0)
            for r in range(ROW_CHUNKS):
                hidden(1 - r, j if r else before, slot if r else 1 - slot)
                both_s[r] = dot(a_s[pl.ds(r * ROWS, ROWS), :], wgu_t[slot])
                if r == 0:
                    pl.when(j >= 1)(lambda: start(stores(j - 1, 1 - slot)))
                    pl.when(j >= 2)(lambda: wait(stores(j - 2, slot)))
                gather.events(done_by(2 * j + r), done_by(2 * j + r + 1))

        def hidden(r, j, slot):
            rows = pl.ds(r * ROWS, ROWS)
            gate, up = both_s[r, :, pl.ds(0, TILE)], both_s[r, :, pl.ds(TILE, TILE)]
            s = 0.5 * jnp.tanh(0.5 * gate) + 0.5
            q = gate * s
            q_s[slot, rows, :] = q
            p_s[slot, rows, :] = up * (s + q * (1 - s))
            prod = (q * up).astype(BF16)
            pt_s[slot, :, rows] = prod.T
            prod_s[rows, pl.ds(mult(j * TILE, TILE), TILE)] = prod

        loop(0, TILES, tick)
        last = TILES - 1
        hidden(1, last, last % 2)
        start(stores(last, last % 2))
        for j in (last - 1, last):
            wait(stores(j, j % 2))

        @pl.when(l == 0)
        def _():
            gather.wait_unit(UNIT_KINDS.index(DOWN))
            now = READY + 2 * PER_UNIT
            put_at(0).wait()
            add_mlp(now)
            now += ITEMS * ROW_CHUNKS * len(N_PIECES)
            norm(1, now, 1)
            put_h.start()

    norm(0, 2 * ITEMS, 1)
    gather.events(2 * ITEMS + T // CH, READY)
    wait(locals_)
    loop(0, LAYERS, layer)
    put_h.wait()
    put_at(1).wait()


PAIRS, STEPS, PLACES = 4, 8, 4
PER_PAIR = STEPS // 2 * PLACES
QUEUE = LAYERS * PAIRS + 1
SECOND = PAIRS + 1
D_PARTS = ((0, 152), (152, 144))
BIG = 2 * TILE
BIGS = (TILES + 1) // 2
PART_BIGS = 3
C_PART = PART_BIGS * BIG
C_LAST = FF - 2 * C_PART
D_PIECE, C_PIECE = 72, 6 * 128
LAST_EVENT = (QUEUE + 1) * PER_PAIR
AHEAD = PLACES - 1
LAG = 2 * PLACES
BEFORE, BETWEEN, AFTER = (2, 63), (12, 74), (63, 120)


def backward_pass(
    here, gather, dy_ref, x_ref, h1_ref, g_ref, d_ref, p_ref, q_ref, actt_ref, at_ref,
    dx_out, dg_out, du_out, dd_out, terms_gu, terms_d, slot_d, slot_c,
    red_recv, red_send, st_sem, fin_sem, sd_recv, sgu_recv, lhs_sem, blk_sem, blk_send, w_sem, term_sem, term_send, misc_sem,
    dh_s, at_s, h_s, dacc, lhs_t, blk_s, wgu_t, wd_t, p_t, q_t, dz_s, term_s, st_d, st_c,
):
    def chips(s):
        return here.chip_at(-1 - s), here.chip_at(1 + s)

    class Lane:
        def __init__(self, l, pair, lane, s, place, down, last):
            chip, _ = chips(s)
            self.s, self.place, self.lane = s, place, lane
            self.sems = [sem.at[l, pair, lane] for sem in (red_recv, red_send)]
            self.fin = fin_sem.at[l, pair, lane]
            if down:
                first, size = D_PARTS[last]
                rows, cut = pl.ds(first, size), pl.ds(0, size)
                pieces = [pl.ds(0, D_PIECE), pl.ds(D_PIECE, size - D_PIECE)]
                self.slot = slot_d.at[lane, s, cut, :]
                self.slots = [[slot_d.at[lane, to, piece, :] for to in (s, s + 1)] for piece in pieces]
                self.ends = [[st_d.at[place, i, piece, :] for i in range(2)] for piece in pieces]
                self.terms = terms_d.at[:, l, chip, rows, :]
                self.st = st_d.at[place, :, cut, :]
                self.result = dd_out.at[l, rows, :]
            else:
                part = pair - 1
                size = C_LAST if last else C_PART
                cols, cut = (pl.ds(first, size) for first in (mult(part * C_PART, 128), 0))
                pieces = [pl.ds(0, C_PIECE), pl.ds(C_PIECE, size - C_PIECE)]
                self.slot = slot_c.at[part, lane, s, :, cut]
                self.slots = [[slot_c.at[part, lane, to, :, piece] for to in (s, s + 1)] for piece in pieces]
                self.ends = [[st_c.at[place, i, :, piece] for i in range(2)] for piece in pieces]
                self.terms = terms_gu.at[:, l, lane, chip, :, cols]
                self.st = st_c.at[place, :, :, cut]
                self.result = [out.at[l, :, cols] for out in (dg_out, du_out)]

        def stage(self):
            return pltpu.make_async_copy(self.terms, self.st, st_sem.at[self.place])

        def send(self, to, piece):
            recv, sent = self.sems
            src, dst = self.slots[piece][0], self.slots[piece][to]
            return remote(src, dst, sent.at[self.s], recv.at[self.s + to, piece], here.next)

        def finish(self, action):
            if not isinstance(self.result, list):
                action(pltpu.make_async_copy(self.slot, self.result, self.fin))
                return
            for lane, result in enumerate(self.result):
                copy = pltpu.make_async_copy(self.slot, result, self.fin)
                pl.when(self.lane == lane)(functools.partial(action, copy))

        def step(self):
            self.stage().wait()
            for i in range(2):
                slot = self.slots[i][0]
                own, sib = (end[...].astype(F32) for end in self.ends[i])
                total = own + sib

                @pl.when(self.s > 0)
                def _():
                    self.send(0, i).wait_recv()
                    slot[...] = (slot[...].astype(F32) + total).astype(BF16)

                @pl.when(self.s == 0)
                def _():
                    slot[...] = total.astype(BF16)

                pl.when(self.s < STEPS - 1)(lambda: self.send(1, i).start())
            pl.when(self.s == STEPS - 1)(lambda: self.finish(lambda copy: copy.start()))

        def wait_out(self):
            recv, sent = self.sems
            both = remote(self.slot, self.slot, sent.at[self.s], recv.at[self.s, 0], here.next)
            pl.when(self.s < STEPS - 1)(both.wait_send)
            pl.when(self.s == STEPS - 1)(lambda: self.finish(lambda copy: copy.wait()))

        def prefetch(self):
            self.stage().start()

    def with_lane(e, action, ahead_of=lambda l, pair, lane, s: None):
        round_, place = e // PLACES, lax.rem(e, PLACES)
        new = place // 2
        index = round_ // PLACES + new - 1
        s = lax.rem(round_, PLACES) + PLACES * (1 - new)
        lane = lax.rem(place, 2)

        @pl.when((index >= 0) & (index < QUEUE) & (index != 1))
        def _():
            second = jnp.where(index < SECOND, 0, 1)
            free = jnp.where((index > 1) & (index < SECOND), 1, 0)
            l, pair = 1 - second, index - SECOND * second - free
            ahead_of(l, pair, lane, s)
            for is_down, is_last, chosen in (
                (True, False, (pair == 0) & (lane == 0)), (True, True, (pair == 0) & (lane == 1)),
                (False, False, (pair > 0) & (pair < PAIRS - 1)), (False, True, pair == PAIRS - 1),
            ):
                pl.when(chosen)(lambda: action(Lane(l, pair, lane, s, place, is_down, is_last)))

    def terms_ready(l, pair, lane, s):
        @pl.when((pair == 0) & (lane == 0))
        def _():
            whole = terms_d.at[1, l, 0]
            remote(whole, whole, blk_send.at[0], sd_recv.at[l, s], here.sibling).wait_recv()

        @pl.when((pair > 0) & (lane == 0) & (s == 0))
        def _():
            for is_last in (False, True):
                width = FFP - 2 * C_PART if is_last else C_PART

                @pl.when((pair == PAIRS - 1) == is_last)
                def _(width=width):
                    part = terms_gu.at[1, l, :, :, :, pl.ds(0, width)]
                    sem = sgu_recv.at[l, pair - 1]
                    remote(part, part, term_send.at[0, 0], sem, here.sibling).wait_recv()

    def events(lo, hi):
        loop(lo, hi, event)

    def fetch(e):
        with_lane(e, Lane.prefetch, terms_ready)

    def event(e):
        pl.when(e >= LAG)(lambda: with_lane(e - LAG, Lane.wait_out))
        fetch(e + AHEAD)
        with_lane(e, Lane.step)

    def lhs_loads(l, s, slot):
        mine, other = chips(s)
        rows = ((mine * 2 + here.core) * RD, (other * 2 + 1 - here.core) * RD)
        return [
            pltpu.make_async_copy(actt_ref.at[l, pl.ds(mult(row, 8), RD), :], lhs_t.at[slot, i], lhs_sem.at[slot, i])
            for i, row in enumerate(rows)
        ]

    def block_copies(l, s, slot):
        mine, other = chips(s)
        return (
            pltpu.make_async_copy(blk_s.at[slot, 0], terms_d.at[0, l, mine], blk_sem.at[slot]),
            remote(blk_s.at[slot, 1], terms_d.at[1, l, other], blk_send.at[slot], sd_recv.at[l, s], here.sibling),
        )

    def both_halves(j, action):
        action(0)
        pl.when(j < BIGS - 1)(lambda: action(1))

    def tile_loads(l, j, slot, half):
        tile = 2 * j + half
        src = pl.ds(mult(tile * TILE, TILE), TILE)
        dst = pl.ds(half * TILE, TILE)
        pairs = [
            (d_ref.at[l, src, :], wd_t.at[slot, dst, :]),
            (p_ref.at[l, tile], p_t.at[slot, :, dst]),
            (q_ref.at[l, tile], q_t.at[slot, :, dst]),
        ]
        pairs += [(g_ref.at[l, m, :, src], wgu_t.at[slot, :, pl.ds((2 * half + m) * TILE, TILE)]) for m in range(2)]
        return [pltpu.make_async_copy(src, dst, w_sem.at[slot, half, i]) for i, (src, dst) in enumerate(pairs)]

    def term_copies(l, j, half):
        cols = pl.ds(mult((2 * j + half) * TILE, TILE), TILE)
        part = jnp.minimum(j // PART_BIGS, PAIRS - 2)
        own, sib = [], []
        for m in range(2):
            mine, other = term_s.at[half, m, :, here.core], term_s.at[half, m, :, 1 - here.core]
            own.append(pltpu.make_async_copy(mine, terms_gu.at[0, l, m, :, :, cols], term_sem.at[half, m]))
            to = terms_gu.at[1, l, m, :, :, cols]
            sib.append(remote(other, to, term_send.at[half, m], sgu_recv.at[l, part], here.sibling))
        return own, sib

    def start_terms(l, j, half):
        own, sib = term_copies(l, j, half)
        start(own + sib)

    def wait_terms(l, j, half):
        own, sib = term_copies(l, j, half)
        wait(own)
        for copy in sib:
            copy.wait_send()

    def wait_block(l, s, slot):
        own, sib = block_copies(l, s, slot)
        own.wait()
        sib.wait_send()

    def layer(i):
        l = 1 - i
        before, between, after = (jnp.where(i == 0, *counts) for counts in (BEFORE, BETWEEN, AFTER))
        load_at = pltpu.make_async_copy(at_ref.at[l], at_s, misc_sem.at[0])
        load_at.start()
        pl.when(i == 0)(pltpu.make_async_copy(h1_ref, h_s, misc_sem.at[1]).start)
        pl.when(i == 1)(pltpu.make_async_copy(x_ref, h_s, misc_sem.at[1]).start)
        for s in range(2):
            start(lhs_loads(l, s, s))
        first_loads = lambda: both_halves(0, lambda half: start(tile_loads(l, 0, 0, half)))
        pl.when(i == 1)(first_loads)

        def pair(s):
            slot = lax.rem(s, 2)
            there = lax.rem(s, 3)
            pl.when(s < STEPS - 2)(lambda: start(lhs_loads(l, s + 2, lax.rem(s + 2, 3))))
            wait(lhs_loads(l, s, there))
            for b in range(2):
                blk_s[slot, b] = dot(lhs_t[there, b], dh_s[...]).astype(BF16)
            start(block_copies(l, s, slot))

            @pl.when(i == 0)
            def _():
                lo, hi = (FORWARD_END + (GATHER_END - FORWARD_END) * to // STEPS for to in (s, s + 1))
                gather.events(lo, hi)

            pl.when(s >= 1)(lambda: wait_block(l, s - 1, 1 - slot))
            pl.when((i == 0) & (s == 1))(lambda: loop(BEFORE[0], BEFORE[0] + AHEAD, fetch))

            def done_by(s):
                cap = jnp.where(i == 0, jnp.maximum(PLACES * s - 1, before), LAST_EVENT)
                return jnp.minimum(before + ((between - before) * (s + 1)) // STEPS, cap)

            loop(jnp.where(s == 0, before, done_by(s - 1)), done_by(s), event)

        loop(0, STEPS, pair)
        wait_block(l, STEPS - 1, (STEPS - 1) % 2)

        @pl.when(i == 0)
        def _():
            gather.wait_unit(UNITS - 1)
            first_loads()

        load_at.wait()
        dacc[...] = jnp.zeros_like(dacc)

        def tick(j):
            slot = lax.rem(j, 2)
            pl.when(j + 1 < BIGS)(lambda: both_halves(j + 1, lambda half: start(tile_loads(l, j + 1, 1 - slot, half))))
            both_halves(j, lambda half: wait(tile_loads(l, j, slot, half)))

            @pl.when(j == BIGS - 1)
            def _():
                for ref in (p_t, q_t):
                    ref[slot, :, pl.ds(TILE, TILE)] = jnp.zeros((T, TILE), F32)

            def done_by(k):
                ready = jnp.maximum(k - 2, 0) // (PART_BIGS * 4)
                cap = jnp.where(i == 0, PER_PAIR * (2 + jnp.minimum(ready, PAIRS - 2)) - 1, LAST_EVENT)
                return jnp.minimum(between + (k * (after - between)) // (4 * BIGS), cap)

            def quarter(k):
                events(done_by(4 * j + k), done_by(4 * j + k + 1))

            for r in range(2):
                rows = pl.ds(r * ROWS, ROWS)
                dprod = dot(dh_s[rows, :], wd_t[slot], ((1,), (1,))).astype(BF16).astype(F32)
                by_gate = (dprod * p_t[slot, rows, :]).astype(BF16)
                by_up = (dprod * q_t[slot, rows, :]).astype(BF16)
                for half in range(2):
                    for m, by in enumerate((by_gate, by_up)):
                        part = by[:, half * TILE : (half + 1) * TILE]
                        dz_s[rows, pl.ds((2 * half + m) * TILE, TILE)] = part
                dacc[rows, :] += dot(dz_s[rows, :], wgu_t[slot], ((1,), (1,)))
                if r == 1:
                    pl.when(j > 0)(lambda: [wait_terms(l, j - 1, half) for half in range(2)] and None)
                quarter(r)
            for r in range(2):
                term = dot(at_s[pl.ds(r * D // 2, D // 2), :], dz_s[...])
                for b in range(8):
                    for half in range(2):
                        for m in range(2):
                            col = (2 * half + m) * TILE
                            block = term[b * RG : (b + 1) * RG, col : col + TILE]
                            term_s[half, m, r * 4 + b // 2, b % 2] = block.astype(BF16)
                if r == 1:
                    both_halves(j, lambda half: start_terms(l, j, half))
                quarter(2 + r)

        loop(0, BIGS, tick)
        wait_terms(l, BIGS - 1, 0)
        pltpu.make_async_copy(h1_ref, h_s, misc_sem.at[1]).wait()

        def new_dh(r):
            rows = pl.ds(mult(r * CH, CH), CH)
            da = dacc[rows, :].astype(BF16).astype(F32)
            wide = h_s[rows, :].astype(F32)
            scale = lax.rsqrt(jnp.mean(wide * wide, -1, keepdims=True) + EPS)
            along = jnp.mean(da * wide, -1, keepdims=True) * scale * scale
            by_h = (scale * (da - wide * along)).astype(BF16).astype(F32)
            dh_s[rows, :] = (dh_s[rows, :].astype(F32) + by_h).astype(BF16)

        loop(0, T // CH, new_dh)

    load_dy = pltpu.make_async_copy(dy_ref, dh_s, misc_sem.at[2])
    load_dy.start()
    load_dy.wait()
    loop(0, LAYERS, layer)
    put_dx = pltpu.make_async_copy(dh_s, dx_out, misc_sem.at[2])
    put_dx.start()
    loop(AFTER[1], LAST_EVENT, event)
    loop(LAST_EVENT - LAG, LAST_EVENT, lambda e: with_lane(e, Lane.wait_out))
    put_dx.wait()


def kernel(
    dy_ref, x_ref, wg_ref, wu_ref, wd_ref,
    dx_out, dg_out, du_out, dd_out, terms_gu, terms_d, g_out, d_out, p_out, q_out, actt_out, at_out, h1_out,
    slot_d, slot_c, *sems,
):
    gather_sems, forward_sems, backward_sems = sems[:6], sems[6:11], sems[11:]
    here = Place()
    barrier((here.next, here.prev, here.sibling, here.other))
    gather = Gather(here, (wg_ref, wu_ref, wd_ref), g_out, d_out, gather_sems)
    vmem = pltpu.VMEM
    two = (2, 2)
    pl.run_scoped(
        functools.partial(
            forward_pass, here, gather, x_ref, g_out, d_out, p_out, q_out, actt_out, at_out, h1_out, *forward_sems
        ),
        vmem((T, D), BF16),
        vmem((T, D), BF16),
        vmem((D, T), BF16),
        vmem((T, FFP), BF16),
        vmem((FFP, D), BF16),
        vmem((2, D, 2 * TILE), BF16),
        vmem((2, ROWS, 2 * TILE), F32),
        vmem((2, T, TILE), F32),
        vmem((2, T, TILE), F32),
        vmem((2, TILE, T), BF16),
        vmem((D, FFP - FF), BF16),
        vmem((FFP - FF, D), BF16),
    )
    pl.run_scoped(
        functools.partial(
            backward_pass, here, gather, dy_ref, x_ref, h1_out, g_out, d_out, p_out, q_out, actt_out, at_out,
            dx_out, dg_out, du_out, dd_out, terms_gu, terms_d, slot_d, slot_c, *backward_sems,
        ),
        vmem((T, D), BF16),
        vmem((D, T), BF16),
        vmem((T, D), BF16),
        vmem((T, D), F32),
        vmem((3, 2, RD, T), BF16),
        vmem((*two, RD, D), BF16),
        vmem((2, D, 2 * BIG), BF16),
        vmem((2, BIG, D), BF16),
        vmem((2, T, BIG), F32),
        vmem((2, T, BIG), F32),
        vmem((T, 2 * BIG), BF16),
        vmem((*two, 8, 2, RG, TILE), BF16),
        vmem((PLACES, 2, D_PARTS[0][1], D), BF16),
        vmem((PLACES, 2, RG, C_LAST), BF16),
    )
    for u in range(UNITS):
        gather.wait_sends(u)


def both_passes(dy, x, wg, wu, wd):
    any_, vmem = pl.BlockSpec(memory_space=pl.ANY), pl.BlockSpec(memory_space=pltpu.VMEM)
    dma = pltpu.SemaphoreType.DMA
    shape = jax.ShapeDtypeStruct
    two = (2, 2)
    per_part = (LAYERS, PAIRS, 2)
    outs = (
        shape((T, D), BF16),
        *[shape((LAYERS, RG, FF), BF16)] * 2,
        shape((LAYERS, RD, D), BF16),
        shape((2, LAYERS, 2, 8, RG, FFP), BF16),
        shape((2, LAYERS, 8, RD, D), BF16),
        shape((LAYERS, 2, D, FFP), BF16),
        shape((LAYERS, FFP, D), BF16),
        *[shape((LAYERS, TILES, T, TILE), F32)] * 2,
        shape((LAYERS, FFP, T), BF16),
        shape((LAYERS, D, T), BF16),
        shape((T, D), BF16),
    )
    gather_sems = [dma((UNITS, HOPS, ITEMS)), dma((UNITS, HOPS)), *[dma((UNITS,))] * 4]
    forward_sems = [dma((LAYERS * 6,)), dma(two), dma((2, 3)), dma((2,)), dma((2,))]
    backward_sems = [
        dma((*per_part, STEPS, 2)),
        dma((*per_part, STEPS)),
        dma((PLACES,)),
        dma(per_part),
        dma((LAYERS, STEPS)),
        dma((LAYERS, PAIRS - 1)),
        dma((3, 2)),
        dma((2,)),
        dma((2,)),
        dma((*two, 5)),
        dma(two),
        dma(two),
        dma((3,)),
    ]
    return pl.pallas_call(
        kernel,
        out_shape=outs,
        in_specs=[any_] * 2 + [vmem] * 3,
        out_specs=(any_,) * len(outs),
        scratch_shapes=[
            pltpu.VMEM((2, STEPS, D_PARTS[0][1], D), BF16),
            pltpu.VMEM((PAIRS - 1, 2, STEPS, RG, C_LAST), BF16),
            *gather_sems,
            *forward_sems,
            *backward_sems,
        ],
        compiler_params=pltpu.CompilerParams(
            collective_id=0, has_side_effects=True, vmem_limit_bytes=63 * 1024 * 1024
        ),
        name="both_passes",
    )(dy, x, wg, wu, wd)


def solution(mesh):
    def step(x, dy, wg, wu, wd):
        dx, dg, du, dd, *_ = both_passes(dy[0], x[0], wg, wu, wd)
        return dx[None], dg, du, dd

    both, rows = P(("rep", "dp"), None, None), P(None, "dp", None)
    own = P("rep", "dp", None)
    return jax.shard_map(
        step,
        mesh=mesh,
        in_specs=(both, both, rows, rows, rows),
        out_specs=(both, own, own, own),
        check_vma=False,
    )
```
